32 devices in a mesh: grp: 8 (over z, y), row: 4 (over x, core).
Axes of the slice: x: 2, y: 2, z: 4, core: 2. Of those that a mesh axis runs over, the one named last changes fastest.
Arguments:
- block: bfloat16 [8192, 1024], P(('grp', 'row')), may hold values from -6 to 6
- degree: int32 [8192], P(('grp', 'row')), may hold values from 1 to 3
- tile_values: bfloat16 [2048, 128, 128], P(('grp', 'row')), may hold values from -0.1875 to 0.1875
- tile_rows: int32 [2048], P(('grp', 'row')), may hold values from 0 to 1
- tile_cols: int32 [2048], P(('grp', 'row')), may hold values from 0 to 15
- tile_count: int32 [32], P(('grp', 'row')), may hold values from 24 to 64, as said below
- send_tiles: int32 [32, 8], P(('grp', 'row')), may hold values from 0 to 1
Outputs:
- logs: bfloat16 [8192, 1024], P(('grp', 'row'))
- gram: float32 [8192, 1024], P(('grp', 'row'))
The draws below stay inside these ranges and needn't reach their ends.
Inputs may be any that keep to these rules, and one draw needn't show every extreme that they name: Slots of a device at positions tile_count or later are padding; some device has all 64 slots live.
All inputs are finite; a program needn't handle non-finite values.
Results may differ from the reference program's by a relative error of at most 0.014.
Values may be sent and summed in bfloat16 or wider, within the bound.
A program may use at most 128 MiB of HBM per device.

```python
import jax
import jax.numpy as jnp
from jax import lax

K = 1024
TILE = 128
ROWS_DEV = 256
SLOTS = 64
POWERS = 2
ROW_TILES = 2
NODES = 8192
SOURCES = 16
SLOTS_ALL = 2048
N_GRP = 8
N_ROW = 4


def draw_tile_count(key, part):
    first_key, second_key = jax.random.split(jax.random.fold_in(key, 7))
    devices = N_GRP * N_ROW
    drawn = jax.random.randint(first_key, (devices,), 0, SLOTS + 1)
    counts = jnp.minimum(SLOTS * 3 // 8 + drawn * drawn * 5 // (8 * SLOTS), SLOTS)
    chosen = jax.random.randint(second_key, (), 0, devices)
    counts = jnp.where(jnp.arange(devices) == chosen, SLOTS, counts)
    return counts.astype(jnp.int32)


def with_ends(values, stream_key, least, top_value):
    spot = [jax.random.randint(jax.random.fold_in(stream_key, axis), (), 0, length) for axis, length in enumerate(values.shape)]
    longest = values.shape.index(max(values.shape))
    beside = spot[:longest] + [(spot[longest] + 1) % values.shape[longest]] + spot[longest + 1:]
    return values.at[tuple(spot)].set(least).at[tuple(beside)].set(top_value)


def steps_of(key, extent, cuts, low, largest):
    gain, own = 1.0, jax.random.fold_in(key, 6)
    for axis_at, blocks in cuts:
        heights = jnp.exp(jax.random.uniform(jax.random.fold_in(own, axis_at), (blocks,), jnp.float32, low / len(cuts), largest / len(cuts)))
        gain = gain * jnp.repeat(heights, extent[axis_at] // blocks).reshape([-1 if axis == axis_at else 1 for axis in range(len(extent))])
    return gain


def centred(stream_key, extent, spread, reach, cuts=(), kind=jnp.bfloat16):
    gain = steps_of(stream_key, extent, cuts, -0.22, 0.18) if cuts else 1.0
    values = jax.random.normal(stream_key, extent, jnp.float32) * spread * gain
    return jnp.minimum(jnp.maximum(values, -reach), reach).astype(kind)


def setup_inputs(seed: int = 0) -> dict:
    key_of = jax.random.split(jax.random.key(seed), 8)
    return {
        "block": centred(key_of[0], (NODES, K), 1.0, 6.0, ((0, 32),)),
        "degree": with_ends(jax.random.randint(key_of[1], (NODES,), 1, 4), jax.random.fold_in(key_of[1], 1), 1, 3).astype(jnp.int32),
        "tile_values": centred(key_of[2], (SLOTS_ALL, TILE, TILE), (SLOTS * 16) ** -0.5, 0.1875, ((0, 32),)),
        "tile_rows": with_ends(jax.random.randint(key_of[3], (SLOTS_ALL,), 0, ROW_TILES), jax.random.fold_in(key_of[3], 1), 0, ROW_TILES - 1).astype(jnp.int32),
        "tile_cols": with_ends(jax.random.randint(key_of[4], (SLOTS_ALL,), 0, SOURCES), jax.random.fold_in(key_of[4], 1), 0, SOURCES - 1).astype(jnp.int32),
        "tile_count": draw_tile_count(jax.random.fold_in(key_of[7], 71), 0),
        "send_tiles": with_ends(jax.random.randint(key_of[6], (N_GRP * N_ROW, N_GRP), 0, ROW_TILES), jax.random.fold_in(key_of[6], 1), 0, ROW_TILES - 1).astype(jnp.int32),
    }


def column_tiles(tile_cols, send_tiles):
    row_tiles = ROWS_DEV // TILE
    slot_ids = jnp.arange(SLOTS * N_GRP * N_ROW, dtype=jnp.int32)
    device = slot_ids // SLOTS
    group = device // N_ROW
    member = device % N_ROW
    local_span = N_ROW * row_tiles
    source_group = jnp.maximum(tile_cols - local_span, 0)
    source_device = (source_group * N_ROW + member).astype(jnp.int32)
    remote = source_device * row_tiles + send_tiles[source_device, group]
    return jnp.where(tile_cols < local_span, group * local_span + tile_cols, remote).astype(jnp.int32)


def reference(block, degree, tile_values, tile_rows, tile_cols, tile_count, send_tiles):
    devices = N_GRP * N_ROW
    row_tiles = ROWS_DEV // TILE
    columns = column_tiles(tile_cols, send_tiles).reshape(devices, SLOTS)
    values = tile_values.reshape(devices, SLOTS, TILE, TILE)
    rows = tile_rows.reshape(devices, SLOTS)
    tile_ids = jnp.arange(row_tiles, dtype=jnp.int32)
    slot_pos = jnp.arange(SLOTS, dtype=jnp.int32)
    current = block
    power_sum = jnp.zeros(block.shape, jnp.float32)
    for power in range(POWERS):
        tiles_all = current.reshape(-1, TILE, K).astype(jnp.float32)

        def one_device(pieces):
            values_here, columns_here, rows_here, count_here = pieces
            picked = tiles_all[columns_here]
            products = jnp.einsum("sik,skf->sif", values_here.astype(jnp.float32), picked, precision=lax.Precision.HIGHEST)
            live_mask = slot_pos < count_here
            weights = ((rows_here[None, :] == tile_ids[:, None]) & live_mask[None, :]).astype(jnp.float32)
            return jnp.einsum("rs,sif->rif", weights, products, precision=lax.Precision.HIGHEST)

        summed = lax.map(one_device, (values, columns, rows, tile_count))
        current = (summed.reshape(-1, K) / degree[:, None].astype(jnp.float32)).astype(jnp.bfloat16)
        power_sum = power_sum + current.astype(jnp.float32)
    logs = jnp.log(jnp.maximum(3.0 * power_sum, 1.0)).astype(jnp.bfloat16)
    grouped = logs.reshape(N_GRP, N_ROW * ROWS_DEV, K)

    def group_gram(group_logs):
        return jnp.dot(group_logs.T, group_logs, preferred_element_type=jnp.float32)

    gram = lax.map(group_gram, grouped) / (N_ROW * ROWS_DEV)
    return logs, gram.reshape(N_GRP * K, K)
```

```python
import functools

import jax
import jax.numpy as jnp
from jax import lax
from jax.experimental import pallas as pl
from jax.experimental.pallas import tpu as pltpu
from jax.sharding import PartitionSpec as P

POWERS = 2
LINE = 4
CHUNKS = 8
AHEAD = 2
LAG_JOIN = 2
LAG_FINISH = 2
LAG_RELAY = 4
LAG_PASS = 4
MESH = pl.DeviceIdType.MESH


def relays_after(n, first, chunks, steps):
    near = [n + 2] if n + 2 < chunks else []
    later = [m for m in (n + LAG_RELAY,) if chunks <= m < steps]
    if n == first:
        later = [m for m in range(chunks, n + LAG_RELAY) if m < steps] + later
    return near + later


def order_kernel(sources, rows_ref, cols_ref, count_ref, before_ref, last_ref):
    slots = rows_ref.shape[0]

    def clear(place, carry):
        last_ref[place] = slots
        return carry

    def skip(slot, carry):
        before_ref[slot] = slots
        return carry

    def link(slot, carry):
        place = rows_ref[slot] * sources + cols_ref[slot]
        before_ref[slot] = last_ref[place]
        last_ref[place] = slot
        return carry

    lax.fori_loop(0, last_ref.shape[0], clear, 0)
    lax.fori_loop(0, slots, skip, 0)
    lax.fori_loop(0, count_ref[0], link, 0)


def step_kernel(
    groups, ranks, send_ref, before_ref, last_ref, degree_ref, values_hbm, block_ref, logs_ref, gram_ref,
    values_ref, values_sem, sums, near, across, table, given, spread,
    source, line, outgoing, incoming, joint, held, mixed, total, everyone, mine,
    row_send, row_recv, pass_send, up_send, relay_send, line_recv, part_send, part_recv, joint_recv,
    give_send, give_recv, table_send, table_recv,
):
    _, chunks, local, tile, width = source.shape
    row_tiles = line.shape[3]
    rows_here = row_tiles * tile
    lanes = groups // LINE
    g = lax.axis_index("grp")
    r = lax.axis_index("row")
    z = g // lanes
    y = lax.rem(g, lanes)
    half = z // 2
    inner = lax.rem(z + half, 2)
    hub = 1 + half
    far = 2 - half
    end = 3 * half
    far_end = 3 - 3 * half
    onward = hub + inner * (far - hub)
    core = lax.rem(r, 2)
    partner = r + 1 - 2 * core
    pairs = ranks // 2

    slots = values_ref.shape[0]
    load = pltpu.make_async_copy(values_hbm, values_ref, values_sem)
    load.start()

    def at(place, lane):
        return (place * lanes + lane, r)

    def lane_after(step):
        return lax.rem(y + step, lanes)

    def lane_before(step):
        return lax.rem(y + lanes - step, lanes)

    def same_core(step):
        return lax.rem(r + 2 * step, ranks)

    barrier = pltpu.get_barrier_semaphore()
    for step in range(1, groups):
        pl.semaphore_signal(barrier, inc=1, device_id=(lax.rem(g + step, groups), r), device_id_type=MESH)
    for step in range(1, ranks):
        pl.semaphore_signal(barrier, inc=1, device_id=(g, lax.rem(r + step, ranks)), device_id_type=MESH)

    def remote(src, dst, send_sem, recv_sem, to):
        return pltpu.make_async_remote_copy(
            src_ref=src, dst_ref=dst, send_sem=send_sem, recv_sem=recv_sem, device_id=to, device_id_type=MESH)

    def land(phase, j, rank):
        where = pl.ds(rank * row_tiles, row_tiles)
        return source.at[phase, j, where] if phase < POWERS else everyone.at[j, where]

    def row_copy(phase, j, to):
        spot = land(phase, j, r)
        return remote(spot, spot, row_send.at[phase, j, to], row_recv.at[phase, j, r], (g, to))

    def pass_copy(phase, j, rank):
        spot = land(phase, j, rank)
        return remote(spot, spot, pass_send.at[phase, j, rank], row_recv.at[phase, j, rank], (g, partner))

    def up_copy(phase, j):
        return remote(
            land(phase, j, r), line.at[phase, j, z], up_send.at[phase, j], line_recv.at[phase, j, z],
            at(onward, y))

    def relay_copy(phase, j):
        spot = line.at[phase, j, end]
        return remote(spot, spot, relay_send.at[phase, j], line_recv.at[phase, j, end], at(far, y))

    def line_arrival(phase, j, place):
        spot = line.at[phase, j, place]
        return remote(spot, spot, relay_send.at[phase, j], line_recv.at[phase, j, place], at(far, y))

    def joined(j):
        return j % 2 == 0

    def part_copy(phase, j, side, step):
        if side and step and joined(j):
            return remote(
                outgoing.at[j, side, step], joint.at[phase, j // 2, step],
                part_send.at[phase, j, side, step], joint_recv.at[phase, j // 2, step],
                at(hub, lane_after(step)))
        return remote(
            outgoing.at[j, side, step], incoming.at[phase, j, step],
            part_send.at[phase, j, side, step], part_recv.at[phase, j, step],
            at(end if side else hub, lane_after(step)))

    def give_copy(side, step):
        return remote(
            across.at[lane_before(step)], given.at[side, step],
            give_send.at[step], give_recv.at[side, step], at(hub, lane_before(step)))

    def table_copy(to):
        return remote(table.at[z], table.at[z], table_send.at[to], table_recv.at[z], at(to, y))

    def table_arrival(place):
        return remote(table.at[place], table.at[place], table_send.at[place], table_recv.at[place], at(far, y))

    def keep(phase, j, value):
        tiles = value.reshape(row_tiles, tile, width)
        if phase < POWERS:
            source[phase, j, pl.ds(r * row_tiles, row_tiles)] = tiles
            line[phase, j, z] = tiles
        else:
            everyone[j, pl.ds(r * row_tiles, row_tiles)] = tiles

    def row_start(phase, j):
        for step in range(1, pairs):
            row_copy(phase, j, same_core(step)).start()
        row_copy(phase, j, partner).start()

    def row_pass(phase, j):
        for step in range(1, pairs):
            rank = lax.rem(r + ranks - 2 * step, ranks)
            pass_copy(phase, j, rank).wait_recv()
            pass_copy(phase, j, rank).start()

    def row_wait(phase, j):
        pass_copy(phase, j, partner).wait_recv()
        for step in range(1, pairs):
            pass_copy(phase, j, lax.rem(partner + ranks - 2 * step, ranks)).wait_recv()

    for group in range(groups):
        tile_of = jnp.full((1, table.shape[2]), send_ref[0, group], jnp.int32)
        table[z, group : group + 1, :] = tile_of.astype(jnp.float32)
    for j in range(chunks):
        keep(0, j, block_ref[:, j * width : (j + 1) * width])

    def clear(slot, carry):
        sums[slot] = jnp.zeros(sums.shape[1:], jnp.float32)
        return carry

    def add_slot(slot, carry):
        sums[slot] = sums[before_ref[slot]] + values_ref[slot].astype(jnp.float32)
        return carry

    lax.fori_loop(0, slots + 1, clear, 0)
    load.wait()
    lax.fori_loop(0, slots, add_slot, 0)
    scales = []
    for row in range(row_tiles):
        degree = degree_ref[row : row + 1, :].astype(jnp.float32)
        scales.append((1.0 / jnp.broadcast_to(degree, (tile, tile))).T)

    def part_of(row, col):
        return (sums[last_ref[row * (local + groups) + col]] * scales[row]).astype(jnp.bfloat16)

    for lane in range(lanes):
        for place in range(LINE):
            for row in range(row_tiles):
                across[lane, row * tile : (row + 1) * tile, place * tile : (place + 1) * tile] = part_of(
                    row, local + place * lanes + lane)

    pl.semaphore_wait(barrier, groups + ranks - 2)
    table_copy(far).start()
    for j in range(min(AHEAD, chunks)):
        up_copy(0, j).start()

    @pl.when(inner == 0)
    def _():
        table_copy(hub).start()
        for step in range(lanes):
            give_copy(1, step).start()
        for j in range(min(AHEAD, chunks), chunks):
            up_copy(0, j).start()

    @pl.when(inner == 1)
    def _():
        for step in range(1, lanes):
            give_copy(0, step).start()

    for j in range(chunks):
        row_start(0, j)
    for row in range(row_tiles):
        for col in range(local):
            near[row * tile : (row + 1) * tile, col * tile : (col + 1) * tile] = part_of(row, col)

    def finish(phase, j, in_line):
        row_wait(phase, j)
        summed = jnp.dot(
            near[...], source[phase, j].reshape(-1, width), preferred_element_type=jnp.float32)
        if in_line:
            summed += held[j]
        for step in range(1, lanes) if in_line else range(1 if joined(j) else lanes):
            remote(
                incoming.at[phase, j, step], incoming.at[phase, j, step], part_send.at[phase, j, 0, step],
                part_recv.at[phase, j, step], at(hub, y)).wait_recv()
            summed += incoming[phase, j, step].astype(jnp.float32)
        current = summed.astype(jnp.bfloat16)
        if phase == 0:
            total[j] = current.astype(jnp.float32)
        else:
            total[j] += current.astype(jnp.float32)
        if phase < POWERS - 1:
            keep(phase + 1, j, current)
            up_copy(phase + 1, j).start()
        else:
            logs = jnp.log(jnp.maximum(3.0 * total[j], 1.0)).astype(jnp.bfloat16)
            logs_ref[:, j * width : (j + 1) * width] = logs
            keep(phase + 1, j, logs)
        row_start(phase + 1, j)

    def relay(phase, j):
        line_arrival(phase, j, end).wait_recv()
        relay_copy(phase, j).start()

    def widen(side, step):
        target = (end if side else hub) * lanes + lane_after(step)
        for place in range(LINE):
            row = table[place, pl.ds(target, 1), :]
            piece = given[side, step, :, place * tile : (place + 1) * tile]
            for kind in range(row_tiles):
                chosen = jnp.where(row == float(kind), 1.0, 0.0).astype(jnp.bfloat16)
                spot = (place * row_tiles + kind) * tile
                spread[side, step, :, spot : spot + tile] = piece * chosen

    def partial(phase, j, sides):
        if sides[0] == 0:
            line_arrival(phase, j, far).wait_recv()
            line_arrival(phase, j, far_end).wait_recv()
        matrix = spread[sides[0] : sides[-1] + 1].reshape(-1, spread.shape[-1])
        summed = jnp.dot(matrix, line[phase, j].reshape(-1, width), preferred_element_type=jnp.float32)
        for side in sides:
            for step in reversed(range(lanes)):
                spot = ((side - sides[0]) * lanes + step) * rows_here
                here = summed[spot : spot + rows_here]
                if side == 0 and step == 0:
                    held[j] = here
                elif step == 0 and joined(j):
                    mixed[j // 2] = here
                else:
                    if phase > 0:
                        part_copy(phase - 1, j, side, step).wait_send()
                    outgoing[j, side, step] = here.astype(jnp.bfloat16)
                    part_copy(phase, j, side, step).start()

    def join(phase, j):
        if joined(j):
            summed = mixed[j // 2]
            for step in range(1, lanes):
                spot = joint.at[phase, j // 2, step]
                remote(
                    spot, spot, part_send.at[phase, j, 1, step], joint_recv.at[phase, j // 2, step],
                    at(hub, y)).wait_recv()
                summed += joint[phase, j // 2, step].astype(jnp.float32)
            if phase > 0:
                part_copy(phase - 1, j, 1, 0).wait_send()
            outgoing[j, 1, 0] = summed.astype(jnp.bfloat16)
            part_copy(phase, j, 1, 0).start()

    def take(side):
        for step in range(1 - side, lanes):
            remote(
                given.at[side, step], given.at[side, step], give_send.at[step], give_recv.at[side, step],
                at(hub, y)).wait_recv()
        for step in range(lanes):
            widen(side, step)

    @pl.when(inner == 1)
    def _():
        given[0, 0] = across[y]
        first = min(AHEAD, chunks)
        for j in range(first):
            relay(0, j)
        for j in range(first, chunks):
            up_copy(0, j).start()
        for j in range(first):
            row_pass(0, j)
        for place in (far, end, far_end):
            table_arrival(place).wait_recv()
        take(0)
        for j in range(first):
            partial(0, j, (0,))
        for j in range(first):
            finish(0, j, True)
        take(1)
        for j in range(first):
            partial(0, j, (1,))
        for j in range(first, chunks):
            row_pass(0, j)
        steps = POWERS * chunks
        for n in range(first, min(first + 2, steps)):
            relay(n // chunks, n % chunks)
        for n in range(first, steps + LAG_PASS):
            if n < steps:
                partial(n // chunks, n % chunks, (0, 1))
            m = n - LAG_JOIN
            if 0 <= m < steps:
                join(m // chunks, m % chunks)
            m = n - LAG_FINISH
            if first <= m < steps:
                finish(m // chunks, m % chunks, True)
            for m in relays_after(n, first, chunks, steps):
                relay(m // chunks, m % chunks)
            m = n - LAG_PASS
            if 0 <= m < steps:
                row_pass(m // chunks + 1, m % chunks)
        for phase in range(POWERS):
            for j in range(chunks):
                relay_copy(phase, j).wait_send()
        for j in range(chunks):
            for side in (0, 1):
                for step in range(1 - side, lanes):
                    part_copy(POWERS - 1, j, side, step).wait_send()
        for step in range(1, lanes):
            give_copy(0, step).wait_send()

    @pl.when(inner == 0)
    def _():
        for j in range(chunks):
            row_pass(0, j)
        steps = POWERS * chunks
        for n in range(steps + 1):
            if n < steps:
                finish(n // chunks, n % chunks, False)
            if n > 0:
                row_pass((n - 1) // chunks + 1, (n - 1) % chunks)
        for step in range(lanes):
            give_copy(1, step).wait_send()
        table_copy(hub).wait_send()

    table_copy(far).wait_send()
    for j in range(chunks):
        row_wait(POWERS, j)
    each = chunks // ranks
    for k in range(each):
        mine[k * width : (k + 1) * width, :] = everyone[r * each + k].reshape(-1, width).T
    rows_all = rows_here * ranks
    for j in range(chunks):
        part = jnp.dot(mine[...], everyone[j].reshape(-1, width), preferred_element_type=jnp.float32)
        gram_ref[:, j * width : (j + 1) * width] = part / rows_all
    for phase in range(POWERS + 1):
        for j in range(chunks):
            if phase < POWERS:
                up_copy(phase, j).wait_send()
            for step in range(1, pairs):
                row_copy(phase, j, same_core(step)).wait_send()
                pass_copy(phase, j, lax.rem(r + ranks - 2 * step, ranks)).wait_send()
            row_copy(phase, j, partner).wait_send()


def body(block, degree, tile_values, tile_rows, tile_cols, tile_count, send_tiles):
    rows_here, width = block.shape
    tile = tile_values.shape[1]
    row_tiles = rows_here // tile
    ranks = lax.axis_size("row")
    groups = lax.axis_size("grp")
    local = ranks * row_tiles
    lanes = groups // LINE
    sources = local + groups
    smem = pl.BlockSpec(memory_space=pltpu.SMEM)
    vmem = pl.BlockSpec(memory_space=pltpu.VMEM)
    slots = tile_values.shape[0]
    before, last = pl.pallas_call(
        functools.partial(order_kernel, sources),
        out_shape=(
            jax.ShapeDtypeStruct((slots,), jnp.int32),
            jax.ShapeDtypeStruct((row_tiles * sources,), jnp.int32),
        ),
        in_specs=[smem, smem, smem],
        out_specs=(smem, smem),
        name="order",
    )(tile_rows, tile_cols, tile_count)
    share = width // ranks
    chunks = max(ranks, CHUNKS)
    part = width // chunks
    dma = pltpu.SemaphoreType.DMA
    half = jnp.bfloat16
    logs, gram = pl.pallas_call(
        functools.partial(step_kernel, groups, ranks),
        out_shape=(
            jax.ShapeDtypeStruct((rows_here, width), half),
            jax.ShapeDtypeStruct((share, width), jnp.float32),
        ),
        in_specs=[smem, smem, smem, vmem, pl.BlockSpec(memory_space=pl.ANY), vmem],
        out_specs=(vmem, vmem),
        scratch_shapes=[
            pltpu.VMEM(tile_values.shape, half),
            dma,
            pltpu.VMEM((slots + 1, tile, tile), jnp.float32),
            pltpu.VMEM((rows_here, local * tile), half),
            pltpu.VMEM((lanes, rows_here, LINE * tile), half),
            pltpu.VMEM((LINE, groups, tile), jnp.float32),
            pltpu.VMEM((2, lanes, rows_here, LINE * tile), half),
            pltpu.VMEM((2, lanes, rows_here, LINE * row_tiles * tile), half),
            pltpu.VMEM((POWERS, chunks, local, tile, part), half),
            pltpu.VMEM((POWERS, chunks, LINE, row_tiles, tile, part), half),
            pltpu.VMEM((chunks, 2, lanes, rows_here, part), half),
            pltpu.VMEM((POWERS, chunks, lanes, rows_here, part), half),
            pltpu.VMEM((POWERS, chunks // 2, lanes, rows_here, part), half),
            pltpu.VMEM((chunks, rows_here, part), jnp.float32),
            pltpu.VMEM((chunks // 2, rows_here, part), jnp.float32),
            pltpu.VMEM((chunks, rows_here, part), jnp.float32),
            pltpu.VMEM((chunks, local, tile, part), half),
            pltpu.VMEM((share, rows_here * ranks), half),
            dma((POWERS + 1, chunks, ranks)),
            dma((POWERS + 1, chunks, ranks)),
            dma((POWERS + 1, chunks, ranks)),
            dma((POWERS, chunks)),
            dma((POWERS, chunks)),
            dma((POWERS, chunks, LINE)),
            dma((POWERS, chunks, 2, lanes)),
            dma((POWERS, chunks, lanes)),
            dma((POWERS, chunks // 2, lanes)),
            dma((lanes,)),
            dma((2, lanes)),
            dma((LINE,)),
            dma((LINE,)),
        ],
        compiler_params=pltpu.CompilerParams(
            collective_id=0, has_side_effects=True, vmem_limit_bytes=67043328),
        name="step",
    )(send_tiles, before, last, degree.reshape(row_tiles, tile), tile_values, block)
    return logs, gram


def solution(mesh):
    placed = (
        P(("grp", "row"), None),
        P(("grp", "row")),
        P(("grp", "row"), None, None),
        P(("grp", "row")),
        P(("grp", "row")),
        P(("grp", "row")),
        P(("grp", "row"), None),
    )
    return jax.shard_map(
        body,
        mesh=mesh,
        in_specs=placed,
        out_specs=(P(("grp", "row"), None), P(("grp", "row"), None)),
        check_vma=False,
    )
```

```python
import functools

import jax
import jax.numpy as jnp
from jax import lax
from jax.experimental import pallas as pl
from jax.experimental.pallas import tpu as pltpu
from jax.sharding import PartitionSpec as P

POWERS = 2
LINE = 4
CHUNKS = 8
AHEAD_HUB = 3
AHEAD_END = 4
FORWARD = 3
LAG_FINISH = 2
LAG_RELAY = 4
AHEAD_RELAY = 3
LAG_PASS = 4
LAG_END = 3
MESH = pl.DeviceIdType.MESH


def relays_after(n, first, chunks, steps):
    near = range(min(AHEAD_END, chunks) if first else n + AHEAD_RELAY, n + AHEAD_RELAY + 1)
    later = range(chunks if first else n + LAG_RELAY, n + LAG_RELAY + 1)
    return [m for m in near if m < chunks] + [m for m in later if chunks <= m < steps]


def order_kernel(sources, rows_ref, cols_ref, count_ref, before_ref, last_ref):
    slots = rows_ref.shape[0]

    def clear(place, carry):
        last_ref[place] = slots
        return carry

    def skip(slot, carry):
        before_ref[slot] = slots
        return carry

    def link(slot, carry):
        place = rows_ref[slot] * sources + cols_ref[slot]
        before_ref[slot] = last_ref[place]
        last_ref[place] = slot
        return carry

    lax.fori_loop(0, last_ref.shape[0], clear, 0)
    lax.fori_loop(0, slots, skip, 0)
    lax.fori_loop(0, count_ref[0], link, 0)


def step_kernel(
    groups, ranks, send_ref, before_ref, last_ref, degree_ref, values_hbm, block_ref, gathered_hbm,
    values_sem, sums, near, across, table, given, spread,
    source, arrived, line, outgoing, incoming, everyone,
    row_send, row_recv, pass_send, up_send, relay_send, line_recv, part_send, part_recv,
    give_send, give_recv, table_send, table_recv, side_send, side_recv, tile_send, tile_recv, out_sem,
):
    chunks, local, tile, width = everyone.shape
    early = arrived.shape[0]
    row_tiles = line.shape[3]
    rows_here = row_tiles * tile
    lanes = groups // LINE
    g = lax.axis_index("grp")
    r = lax.axis_index("row")
    z = g // lanes
    y = lax.rem(g, lanes)
    half = z // 2
    inner = lax.rem(z + half, 2)
    hub = 1 + half
    far = 2 - half
    end = 3 * half
    onward = hub + inner * (far - hub)
    core = lax.rem(r, 2)
    partner = r + 1 - 2 * core
    pairs = ranks // 2

    slots = values_hbm.shape[0]
    load = pltpu.make_async_copy(values_hbm, outgoing.at[pl.ds(0, slots)], values_sem)
    load.start()

    def at(place, lane):
        return (place * lanes + lane, r)

    def lane_after(step):
        return lax.rem(y + step, lanes)

    def lane_before(step):
        return lax.rem(y + lanes - step, lanes)

    def same_core(step):
        return lax.rem(r + 2 * step, ranks)

    barrier = pltpu.get_barrier_semaphore()
    for step in range(1, groups):
        pl.semaphore_signal(barrier, inc=1, device_id=(lax.rem(g + step, groups), r), device_id_type=MESH)
    for step in range(1, ranks):
        pl.semaphore_signal(barrier, inc=1, device_id=(g, lax.rem(r + step, ranks)), device_id_type=MESH)

    def remote(src, dst, send_sem, recv_sem, to):
        return pltpu.make_async_remote_copy(
            src_ref=src, dst_ref=dst, send_sem=send_sem, recv_sem=recv_sem, device_id=to, device_id_type=MESH)

    def land(phase, j, rank):
        where = pl.ds(rank * row_tiles, row_tiles)
        return source.at[phase, j, where] if phase < POWERS else everyone.at[j, where]

    def span(phase, rank):
        where = pl.ds(rank * row_tiles, row_tiles)
        return source.at[phase, :, where] if phase < POWERS else everyone.at[:, where]

    def row_copy(phase, j, step):
        spot = land(phase, j, r)
        to = same_core(step) if step else partner
        arrival = step - 1 if step else pairs - 1
        return remote(spot, spot, row_send.at[phase, step], row_recv.at[phase, j, arrival], (g, to))

    def pass_copy(phase, j, step):
        spot = land(phase, j, lax.rem(r + ranks - 2 * step, ranks))
        return remote(
            spot, spot, pass_send.at[phase, step - 1], row_recv.at[phase, j, pairs - 1], (g, partner))

    def up_copy(phase, j):
        return remote(
            land(phase, j, r), line.at[phase, j, 2 * inner], up_send.at[phase], line_recv.at[phase, j, inner],
            at(onward, y))

    def relay_copy(phase, j):
        return remote(
            line.at[phase, j, 0], line.at[phase, j, 3], relay_send.at[phase], line_recv.at[phase, j, 1],
            at(far, y))

    def line_wait(phase, j, where, kind):
        spot = line.at[phase, j, where]
        remote(spot, spot, relay_send.at[phase], line_recv.at[phase, j, kind], at(far, y)).wait_recv()

    def out_spot(j, side, step):
        return ((j * 2 + side) * lanes + step) * row_tiles

    def side_copy(phase, j, step):
        return remote(
            outgoing.at[out_spot(j, phase, step)], source.at[phase, j, local + step], side_send.at[phase, step],
            side_recv.at[phase, j], at(end, lane_after(step)))

    def tile_copy(j, step, own):
        where = pl.ds(0, 1) if own else pl.ds(1, LINE - 2)
        return remote(
            arrived.at[j, step, where], arrived.at[j, step, where], tile_send.at[1 - own], tile_recv.at[j],
            at(end, lane_after(step)))

    def part_copy(phase, j, side, step):
        return remote(
            outgoing.at[pl.ds(out_spot(j, side, step), row_tiles)], incoming.at[phase, j, step],
            part_send.at[j, side, step], part_recv.at[phase, j],
            at(end if side else hub, lane_after(step)))

    def give_copy(side, step):
        return remote(
            across.at[lane_before(step), side:], given.at[side, step, side:],
            give_send.at[step], give_recv.at[side, step], at(hub, lane_before(step)))

    def table_copy(to, place, sem):
        return remote(table.at[inner], table.at[place], table_send.at[sem], table_recv.at[0], at(to, y))

    def keep(phase, j, value):
        tiles = value.reshape(row_tiles, tile, width)
        if phase < POWERS:
            source[phase, j, pl.ds(r * row_tiles, row_tiles)] = tiles
            line[phase, j, 1] = tiles
        else:
            everyone[j, pl.ds(r * row_tiles, row_tiles)] = tiles

    def wanted(phase, j, group):
        picked = source[phase, j, r * row_tiles]
        for kind in range(1, row_tiles):
            picked = jnp.where(send_ref[0, group] == kind, source[phase, j, r * row_tiles + kind], picked)
        return picked

    def beside(phase, j):
        for step in range(1, lanes):
            outgoing[out_spot(j, phase, step)] = wanted(phase, j, end * lanes + lane_after(step))
            side_copy(phase, j, step).start()
        source[phase, j, local] = wanted(phase, j, g)

    def forward_own(j):
        for step in range(lanes):
            arrived[j, step, 0] = wanted(0, j, end * lanes + lane_after(step))
            tile_copy(j, step, 1).start()

    def forward_rest(j):
        line_wait(0, j, pl.ds(2, 2), 1)
        for step in range(lanes):
            for place in range(2, LINE):
                row = table[place, pl.ds(end * lanes + lane_after(step), 1), :]
                picked = line[0, j, place, 0]
                for kind in range(1, row_tiles):
                    chosen = jnp.where(row == float(kind), 1.0, 0.0).astype(jnp.bfloat16)
                    picked = picked * (1 - chosen) + line[0, j, place, kind] * chosen
                arrived[j, step, place - 1] = picked
            tile_copy(j, step, 0).start()

    def row_start(phase, j):
        for step in (*range(1, pairs), 0):
            row_copy(phase, j, step).start()

    def row_pass(phase, j):
        for step in range(1, pairs):
            rank = lax.rem(r + ranks - 2 * step, ranks)
            spot = land(phase, j, rank)
            remote(spot, spot, row_send.at[phase, 0], row_recv.at[phase, j, step - 1], (g, partner)).wait_recv()
            pass_copy(phase, j, step).start()

    def row_wait(phase, j):
        where = pl.ds(0, pairs * row_tiles)
        spot = source.at[phase, j, where] if phase < POWERS else everyone.at[j, where]
        remote(spot, spot, row_send.at[phase, 0], row_recv.at[phase, j, pairs - 1], (g, partner)).wait_recv()

    for group in range(groups):
        tile_of = jnp.full((1, table.shape[2]), send_ref[0, group], jnp.int32)
        table[inner, group : group + 1, :] = tile_of.astype(jnp.float32)
    for j in range(chunks):
        keep(0, j, block_ref[:, j * width : (j + 1) * width])

    def clear(slot, carry):
        sums[slot] = jnp.zeros(sums.shape[1:], jnp.float32)
        return carry

    def add_slot(slot, carry):
        sums[slot] = sums[before_ref[slot]] + outgoing[slot].astype(jnp.float32)
        return carry

    lax.fori_loop(0, slots + 1, clear, 0)
    load.wait()
    lax.fori_loop(0, slots, add_slot, 0)
    scales = []
    for row in range(row_tiles):
        degree = degree_ref[row : row + 1, :].astype(jnp.float32)
        scales.append((1.0 / jnp.broadcast_to(degree, (tile, tile))).T)

    def part_of(row, col):
        return (sums[last_ref[row * (local + groups) + col]] * scales[row]).astype(jnp.bfloat16)

    for lane in range(lanes):
        for place in range(LINE):
            rank = place + half * (LINE - 1 - 2 * place)
            for row in range(row_tiles):
                across[lane, rank, row * tile : (row + 1) * tile, :] = part_of(row, local + place * lanes + lane)

    pl.semaphore_wait(barrier, groups + ranks - 2)
    table_copy(far, 3 - inner, 0).start()

    @pl.when(inner == 0)
    def _():
        for j in range(min(AHEAD_END, chunks)):
            up_copy(0, j).start()
        table_copy(hub, 0, 1).start()
        for step in range(lanes):
            give_copy(1, step).start()
        for j in range(min(AHEAD_END, chunks), chunks):
            up_copy(0, j).start()

    @pl.when(inner == 1)
    def _():
        for j in range(min(AHEAD_HUB, chunks)):
            up_copy(0, j).start()
        for step in range(1, lanes):
            give_copy(0, step).start()
        for j in range(early):
            forward_own(j)

    for j in range(chunks):
        row_start(0, j)

    @pl.when(inner == 0)
    def _():
        for j in range(chunks):
            beside(0, j)

    for row in range(row_tiles):
        for col in range(local):
            near[row * tile : (row + 1) * tile, col * tile : (col + 1) * tile] = part_of(row, col)
    def finish(phase, j, in_line):
        row_wait(phase, j)
        if in_line:
            kept = sums[pl.ds(j * row_tiles, row_tiles)].reshape(rows_here, width)
            summed = kept + jnp.dot(
                near[...], source[phase, j, :local].reshape(-1, width),
                preferred_element_type=jnp.float32)
        else:
            spot = source.at[phase, j, pl.ds(local + 1, lanes - 1)]
            remote(spot, spot, side_send.at[phase, 0], side_recv.at[phase, j], at(end, y)).wait_recv()
            matrix = jnp.concatenate(
                [near[...]] + [across[lane_before(step), 0] for step in range(lanes)], axis=1)
            summed = jnp.dot(
                matrix, source[phase, j].reshape(-1, width), preferred_element_type=jnp.float32)
        direct = phase == 0 and j < early and not in_line
        if direct:
            spot = arrived.at[j]
            remote(spot, spot, tile_send.at[0], tile_recv.at[j], at(end, y)).wait_recv()
            matrix = jnp.concatenate(
                [across[lane_before(step), place] for step in range(lanes) for place in range(1, LINE)], axis=1)
            summed += jnp.dot(matrix, arrived[j].reshape(-1, width), preferred_element_type=jnp.float32)
        first = lanes if direct else 1 if in_line else 0
        if first < lanes:
            spot = incoming.at[phase, j, pl.ds(first, lanes - first)]
            remote(spot, spot, part_send.at[j, 0, 0], part_recv.at[phase, j], at(hub, y)).wait_recv()
        for step in range(first, lanes):
            summed += incoming[phase, j, step].reshape(rows_here, width).astype(jnp.float32)
        current = summed.astype(jnp.bfloat16)
        if phase < POWERS - 1:
            keep(phase + 1, j, current)
            up_copy(phase + 1, j).start()
            if not in_line:
                beside(phase + 1, j)
        else:
            power_sum = current.astype(jnp.float32)
            for past in range(1, POWERS):
                mine = source[past, j, pl.ds(r * row_tiles, row_tiles)].reshape(rows_here, width)
                power_sum = mine.astype(jnp.float32) + power_sum
            keep(phase + 1, j, jnp.log(jnp.maximum(3.0 * power_sum, 1.0)).astype(jnp.bfloat16))
        row_start(phase + 1, j)

    def relay(phase, j):
        line_wait(phase, j, 0, 0)
        relay_copy(phase, j).start()

    def widen(side, step):
        target = (end if side else hub) * lanes + lane_after(step)
        for place in range(side, LINE):
            row = table[place, pl.ds(target, 1), :]
            piece = given[side, step, place]
            for kind in range(row_tiles):
                chosen = jnp.where(row == float(kind), 1.0, 0.0).astype(jnp.bfloat16)
                spot = (place * row_tiles + kind) * tile
                spread[side, step, :, spot : spot + tile] = piece * chosen

    def partial(phase, j, sides):
        if phase > 0 or j >= early:
            line_wait(phase, j, pl.ds(2, 2), 1)
        for side in sides:
            matrix = spread[side, :, :, side * row_tiles * tile :].reshape(lanes * rows_here, -1)
            summed = jnp.dot(
                matrix, line[phase, j, side:].reshape(-1, width), preferred_element_type=jnp.float32)
            for step in reversed(range(lanes)):
                here = summed[step * rows_here : (step + 1) * rows_here]
                if side == 0 and step == 0:
                    sums[pl.ds(j * row_tiles, row_tiles)] = here.reshape(row_tiles, tile, width)
                else:
                    if phase > 1 or (phase == 1 and (side == 0 or j >= early)):
                        part_copy(phase - 1, j, side, step).wait_send()
                    where = pl.ds(out_spot(j, side, step), row_tiles)
                    outgoing[where] = here.astype(jnp.bfloat16).reshape(row_tiles, tile, width)
                    part_copy(phase, j, side, step).start()

    def take(side):
        for step in range(1 - side, lanes):
            spot = given.at[side, step, side:]
            remote(spot, spot, give_send.at[step], give_recv.at[side, step], at(hub, y)).wait_recv()
        for step in range(lanes):
            widen(side, step)

    @pl.when(inner == 1)
    def _():
        given[0, 0] = across[y]
        sent = min(AHEAD_HUB, chunks)
        for j in range(min(AHEAD_END, chunks)):
            relay(0, j)
            if sent < chunks:
                up_copy(0, sent).start()
                sent += 1
        for j in range(sent, chunks):
            up_copy(0, j).start()
        spot = table.at[pl.ds(0, LINE - 1)]
        remote(spot, spot, table_send.at[0], table_recv.at[0], at(far, y)).wait_recv()
        for j in range(early):
            row_pass(0, j)
        for j in range(early):
            forward_rest(j)
            if j == 0:
                take(0)
            partial(0, j, (0,))
            if j > 0:
                finish(0, j - 1, True)
        for j in range(early, chunks):
            row_pass(0, j)
        take(1)
        steps = POWERS * chunks
        for n in range(early, steps + LAG_PASS):
            if n < steps:
                partial(n // chunks, n % chunks, (0, 1))
            m = n - LAG_FINISH
            if early - 1 <= m < steps:
                finish(m // chunks, m % chunks, True)
            for m in relays_after(n, n == early, chunks, steps):
                relay(m // chunks, m % chunks)
            m = n - LAG_PASS
            if 0 <= m < steps:
                row_pass(m // chunks + 1, m % chunks)
        for own in (0, 1):
            spot = arrived.at[:, :, pl.ds(0, 1) if own else pl.ds(1, LINE - 2)]
            remote(spot, spot, tile_send.at[1 - own], tile_recv.at[0], at(end, y)).wait_send()
        for phase in range(POWERS):
            spot = line.at[phase, :, 0]
            remote(spot, spot, relay_send.at[phase], line_recv.at[phase, 0, 0], at(far, y)).wait_send()
        for j in range(chunks):
            for side in (0, 1):
                for step in range(1 - side, lanes):
                    part_copy(POWERS - 1, j, side, step).wait_send()
        for step in range(1, lanes):
            give_copy(0, step).wait_send()

    @pl.when(inner == 0)
    def _():
        steps = POWERS * chunks
        for j in range(min(AHEAD_END, chunks)):
            row_pass(0, j)
        for n in range(steps + LAG_END):
            if n < steps:
                finish(n // chunks, n % chunks, False)
            if min(AHEAD_END, chunks) + n < chunks:
                row_pass(0, min(AHEAD_END, chunks) + n)
            m = n - LAG_END
            if m >= 0:
                row_pass(m // chunks + 1, m % chunks)
        for step in range(lanes):
            give_copy(1, step).wait_send()
        for phase in range(POWERS):
            for step in range(1, lanes):
                spot = outgoing.at[pl.ds(0, chunks)]
                remote(spot, spot, side_send.at[phase, step], side_recv.at[phase, 0], at(end, y)).wait_send()
        table_copy(hub, 0, 1).wait_send()

    def row_sent(phase):
        for step in range(pairs):
            spot = span(phase, r)
            remote(spot, spot, row_send.at[phase, step], row_recv.at[phase, 0, 0], (g, partner)).wait_send()
        for step in range(1, pairs):
            spot = span(phase, lax.rem(r + ranks - 2 * step, ranks))
            remote(spot, spot, pass_send.at[phase, step - 1], row_recv.at[phase, 0, 0], (g, partner)).wait_send()

    table_copy(far, 3 - inner, 0).wait_send()
    for phase in range(POWERS):
        spot = span(phase, r)
        remote(spot, spot, up_send.at[phase], line_recv.at[phase, 0, 0], at(onward, y)).wait_send()
        row_sent(phase)
    for j in range(chunks):
        row_wait(POWERS, j)
        pltpu.make_async_copy(everyone.at[j], gathered_hbm.at[j], out_sem.at[0]).start()
    row_sent(POWERS)
    pltpu.make_async_copy(everyone, gathered_hbm, out_sem.at[0]).wait()


def gram_kernel(ranks, gathered_hbm, logs_hbm, gram_hbm, gathered, mine, logs, gram, in_sem, logs_sem, out_sem):
    chunks, local, tile, width = gathered.shape
    rows_here = local // ranks * tile
    r = lax.axis_index("row")
    each = chunks // ranks

    def in_copy(j):
        return pltpu.make_async_copy(gathered_hbm.at[j], gathered.at[j], in_sem.at[j])

    def out_copy(k):
        where = pl.ds(pl.multiple_of(k * each * width, width), each * width)
        return pltpu.make_async_copy(gram.at[:, where], gram_hbm.at[:, where], out_sem.at[k])

    def logs_copy(k):
        where = pl.ds(pl.multiple_of(k * each * width, width), each * width)
        return pltpu.make_async_copy(logs.at[:, where], logs_hbm.at[:, where], logs_sem.at[k])

    for j in range(chunks):
        in_copy(lax.rem(r * each + j, chunks)).start()
    for j in range(each):
        in_copy(r * each + j).wait()
        mine[j * width : (j + 1) * width, :] = gathered[r * each + j].reshape(-1, width).T
    own = pl.ds(r * (local // ranks), local // ranks)
    for step in range(ranks):
        k = lax.rem(r + step, ranks)
        if step:
            for j in range(each):
                in_copy(k * each + j).wait()
        block = jnp.concatenate([gathered[k * each + j].reshape(-1, width) for j in range(each)], axis=1)
        part = jnp.dot(mine[...], block, preferred_element_type=jnp.float32) / (rows_here * ranks)
        where = pl.ds(pl.multiple_of(k * each * width, width), each * width)
        gram[:, where] = part
        out_copy(k).start()
        logs[:, where] = jnp.concatenate(
            [gathered[k * each + j, own].reshape(rows_here, width) for j in range(each)], axis=1)
        logs_copy(k).start()
    for k in range(ranks):
        out_copy(k).wait()
        logs_copy(k).wait()


def body(block, degree, tile_values, tile_rows, tile_cols, tile_count, send_tiles):
    rows_here, width = block.shape
    tile = tile_values.shape[1]
    row_tiles = rows_here // tile
    ranks = lax.axis_size("row")
    groups = lax.axis_size("grp")
    local = ranks * row_tiles
    lanes = groups // LINE
    sources = local + groups
    smem = pl.BlockSpec(memory_space=pltpu.SMEM)
    vmem = pl.BlockSpec(memory_space=pltpu.VMEM)
    slots = tile_values.shape[0]
    before, last = pl.pallas_call(
        functools.partial(order_kernel, sources),
        out_shape=(
            jax.ShapeDtypeStruct((slots,), jnp.int32),
            jax.ShapeDtypeStruct((row_tiles * sources,), jnp.int32),
        ),
        in_specs=[smem, smem, smem],
        out_specs=(smem, smem),
        name="order",
    )(tile_rows, tile_cols, tile_count)
    share = width // ranks
    early = max(1, min(FORWARD, 8 // lanes))
    pairs = ranks // 2
    chunks = max(ranks, CHUNKS)
    part = width // chunks
    dma = pltpu.SemaphoreType.DMA
    half = jnp.bfloat16
    anywhere = pl.BlockSpec(memory_space=pl.ANY)
    gathered = pl.pallas_call(
        functools.partial(step_kernel, groups, ranks),
        out_shape=jax.ShapeDtypeStruct((chunks, local, tile, part), half),
        in_specs=[smem, smem, smem, vmem, anywhere, vmem],
        out_specs=anywhere,
        scratch_shapes=[
            dma,
            pltpu.VMEM((slots + 1, tile, tile), jnp.float32),
            pltpu.VMEM((rows_here, local * tile), half),
            pltpu.VMEM((lanes, LINE, rows_here, tile), half),
            pltpu.VMEM((LINE, groups, tile), jnp.float32),
            pltpu.VMEM((2, lanes, LINE, rows_here, tile), half),
            pltpu.VMEM((2, lanes, rows_here, LINE * row_tiles * tile), half),
            pltpu.VMEM((POWERS, chunks, local + lanes, tile, part), half),
            pltpu.VMEM((early, lanes, LINE - 1, tile, part), half),
            pltpu.VMEM((POWERS, chunks, LINE, row_tiles, tile, part), half),
            pltpu.VMEM((chunks * 2 * lanes * row_tiles, tile, part), half),
            pltpu.VMEM((POWERS, chunks, lanes, row_tiles, tile, part), half),
            pltpu.VMEM((chunks, local, tile, part), half),
            dma((POWERS + 1, pairs)),
            dma((POWERS + 1, chunks, pairs)),
            dma((POWERS + 1, pairs)),
            dma((POWERS,)),
            dma((POWERS,)),
            dma((POWERS, chunks, 2)),
            dma((chunks, 2, lanes)),
            dma((POWERS, chunks)),
            dma((lanes,)),
            dma((2, lanes)),
            dma((2,)),
            dma((1,)),
            dma((POWERS, lanes)),
            dma((POWERS, chunks)),
            dma((2,)),
            dma((early,)),
            dma((1,)),
        ],
        compiler_params=pltpu.CompilerParams(
            collective_id=0, has_side_effects=True, vmem_limit_bytes=67043328),
        name="step",
    )(send_tiles, before, last, degree.reshape(row_tiles, tile), tile_values, block)
    return tuple(pl.pallas_call(
        functools.partial(gram_kernel, ranks),
        out_shape=(
            jax.ShapeDtypeStruct((rows_here, width), half),
            jax.ShapeDtypeStruct((share, width), jnp.float32),
        ),
        in_specs=[anywhere],
        out_specs=(anywhere, anywhere),
        scratch_shapes=[
            pltpu.VMEM(gathered.shape, half),
            pltpu.VMEM((share, rows_here * ranks), half),
            pltpu.VMEM((rows_here, width), half),
            pltpu.VMEM((share, width), jnp.float32),
            dma((chunks,)),
            dma((ranks,)),
            dma((ranks,)),
        ],
        name="gram",
    )(gathered))


def solution(mesh):
    placed = (
        P(("grp", "row"), None),
        P(("grp", "row")),
        P(("grp", "row"), None, None),
        P(("grp", "row")),
        P(("grp", "row")),
        P(("grp", "row")),
        P(("grp", "row"), None),
    )
    return jax.shard_map(
        body,
        mesh=mesh,
        in_specs=placed,
        out_specs=(P(("grp", "row"), None), P(("grp", "row"), None)),
        check_vma=False,
    )
```

```python
import functools

import jax
import jax.numpy as jnp
from jax import lax
from jax.experimental import pallas as pl
from jax.experimental.pallas import tpu as pltpu
from jax.sharding import PartitionSpec as P

POWERS = 2
LINE = 4
CHUNKS = 8
AHEAD_HUB = 3
AHEAD_END = 4
FORWARD = 3
LAG_JOIN = 2
LAG_FINISH = 5
LAG_RELAY = 4
AHEAD_RELAY = 3
LAG_PASS = 7
LAG_END = 3
MESH = pl.DeviceIdType.MESH


def relays_after(n, first, chunks, steps):
    near = range(min(AHEAD_END, chunks) if first else n + AHEAD_RELAY, n + AHEAD_RELAY + 1)
    later = range(chunks if first else n + LAG_RELAY, n + LAG_RELAY + 1)
    return [m for m in near if m < chunks] + [m for m in later if chunks <= m < steps]


def order_kernel(sources, rows_ref, cols_ref, count_ref, before_ref, last_ref):
    slots = rows_ref.shape[0]

    def clear(place, carry):
        last_ref[place] = slots
        return carry

    def skip(slot, carry):
        before_ref[slot] = slots
        return carry

    def link(slot, carry):
        place = rows_ref[slot] * sources + cols_ref[slot]
        before_ref[slot] = last_ref[place]
        last_ref[place] = slot
        return carry

    lax.fori_loop(0, last_ref.shape[0], clear, 0)
    lax.fori_loop(0, slots, skip, 0)
    lax.fori_loop(0, count_ref[0], link, 0)


def step_kernel(
    groups, ranks, send_ref, before_ref, last_ref, degree_ref, values_hbm, block_ref, gathered_hbm,
    values_sem, sums, near, across, table, given, spread,
    source, arrived, line, outgoing, incoming, everyone,
    row_send, row_recv, pass_send, up_send, relay_send, line_recv, part_send, part_recv,
    give_send, give_recv, table_send, table_recv, side_send, side_recv, tile_send, tile_recv, joint_recv, out_sem,
):
    chunks, local, tile, width = everyone.shape
    early = arrived.shape[0]
    row_tiles = line.shape[3]
    rows_here = row_tiles * tile
    lanes = groups // LINE
    g = lax.axis_index("grp")
    r = lax.axis_index("row")
    z = g // lanes
    y = lax.rem(g, lanes)
    half = z // 2
    inner = lax.rem(z + half, 2)
    hub = 1 + half
    far = 2 - half
    end = 3 * half
    onward = hub + inner * (far - hub)
    core = lax.rem(r, 2)
    partner = r + 1 - 2 * core
    pairs = ranks // 2

    slots = values_hbm.shape[0]
    load = pltpu.make_async_copy(values_hbm, outgoing.at[pl.ds(0, slots)], values_sem)
    load.start()

    def at(place, lane):
        return (place * lanes + lane, r)

    def lane_after(step):
        return lax.rem(y + step, lanes)

    def lane_before(step):
        return lax.rem(y + lanes - step, lanes)

    def same_core(step):
        return lax.rem(r + 2 * step, ranks)

    barrier = pltpu.get_barrier_semaphore()
    for step in range(1, groups):
        pl.semaphore_signal(barrier, inc=1, device_id=(lax.rem(g + step, groups), r), device_id_type=MESH)
    for step in range(1, ranks):
        pl.semaphore_signal(barrier, inc=1, device_id=(g, lax.rem(r + step, ranks)), device_id_type=MESH)

    def remote(src, dst, send_sem, recv_sem, to):
        return pltpu.make_async_remote_copy(
            src_ref=src, dst_ref=dst, send_sem=send_sem, recv_sem=recv_sem, device_id=to, device_id_type=MESH)

    def land(phase, j, rank):
        where = pl.ds(rank * row_tiles, row_tiles)
        return source.at[phase, j, where] if phase < POWERS else everyone.at[j, where]

    def span(phase, rank):
        where = pl.ds(rank * row_tiles, row_tiles)
        return source.at[phase, :, where] if phase < POWERS else everyone.at[:, where]

    def row_copy(phase, j, step):
        spot = land(phase, j, r)
        to = same_core(step) if step else partner
        arrival = step - 1 if step else pairs - 1
        return remote(spot, spot, row_send.at[phase, step], row_recv.at[phase, j, arrival], (g, to))

    def pass_copy(phase, j, step):
        spot = land(phase, j, lax.rem(r + ranks - 2 * step, ranks))
        return remote(
            spot, spot, pass_send.at[phase, step - 1], row_recv.at[phase, j, pairs - 1], (g, partner))

    def up_copy(phase, j):
        return remote(
            land(phase, j, r), line.at[phase, j, 2 * inner], up_send.at[phase], line_recv.at[phase, j, inner],
            at(onward, y))

    def relay_copy(phase, j):
        return remote(
            line.at[phase, j, 0], line.at[phase, j, 3], relay_send.at[phase], line_recv.at[phase, j, 1],
            at(far, y))

    def line_wait(phase, j, where, kind):
        spot = line.at[phase, j, where]
        remote(spot, spot, relay_send.at[phase], line_recv.at[phase, j, kind], at(far, y)).wait_recv()

    def out_spot(j, side, step):
        return ((j * 2 + side) * lanes + step) * row_tiles

    def side_copy(phase, j, step):
        return remote(
            outgoing.at[out_spot(j, phase, step)], source.at[phase, j, local + step], side_send.at[phase, step],
            side_recv.at[phase, j], at(end, lane_after(step)))

    def tile_copy(j, step, own):
        where = pl.ds(0, 1) if own else pl.ds(1, LINE - 2)
        return remote(
            arrived.at[j, step, where], arrived.at[j, step, where], tile_send.at[1 - own], tile_recv.at[j],
            at(end, lane_after(step)))

    def joined(phase, j):
        return lanes == 2 and phase == POWERS - 1 and j % 2 == 0 and j < chunks - 2

    def part_copy(phase, j, side, step):
        if side and step and joined(phase, j):
            return remote(
                outgoing.at[pl.ds(out_spot(j, side, step), row_tiles)], incoming.at[phase, j, 0],
                part_send.at[j, side, step], joint_recv.at[j], at(hub, lane_after(step)))
        return remote(
            outgoing.at[pl.ds(out_spot(j, side, step), row_tiles)], incoming.at[phase, j, step],
            part_send.at[j, side, step], part_recv.at[phase, j],
            at(end if side else hub, lane_after(step)))

    def give_copy(side, step):
        return remote(
            across.at[lane_before(step), side:], given.at[side, step, side:],
            give_send.at[step], give_recv.at[side, step], at(hub, lane_before(step)))

    def table_copy(to, place, sem):
        return remote(table.at[inner], table.at[place], table_send.at[sem], table_recv.at[0], at(to, y))

    def keep(phase, j, value):
        tiles = value.reshape(row_tiles, tile, width)
        if phase < POWERS:
            source[phase, j, pl.ds(r * row_tiles, row_tiles)] = tiles
            line[phase, j, 1] = tiles
        else:
            everyone[j, pl.ds(r * row_tiles, row_tiles)] = tiles

    def wanted(phase, j, group):
        picked = source[phase, j, r * row_tiles]
        for kind in range(1, row_tiles):
            picked = jnp.where(send_ref[0, group] == kind, source[phase, j, r * row_tiles + kind], picked)
        return picked

    def beside(phase, j):
        for step in range(1, lanes):
            outgoing[out_spot(j, phase, step)] = wanted(phase, j, end * lanes + lane_after(step))
            side_copy(phase, j, step).start()
        source[phase, j, local] = wanted(phase, j, g)

    def forward_own(j):
        for step in range(lanes):
            arrived[j, step, 0] = wanted(0, j, end * lanes + lane_after(step))
            tile_copy(j, step, 1).start()

    def forward_rest(j):
        line_wait(0, j, pl.ds(2, 2), 1)
        for step in range(lanes):
            for place in range(2, LINE):
                row = table[place, pl.ds(end * lanes + lane_after(step), 1), :]
                picked = line[0, j, place, 0]
                for kind in range(1, row_tiles):
                    chosen = jnp.where(row == float(kind), 1.0, 0.0).astype(jnp.bfloat16)
                    picked = picked * (1 - chosen) + line[0, j, place, kind] * chosen
                arrived[j, step, place - 1] = picked
            tile_copy(j, step, 0).start()

    def row_start(phase, j):
        for step in (*range(1, pairs), 0):
            row_copy(phase, j, step).start()

    def row_pass(phase, j):
        for step in range(1, pairs):
            rank = lax.rem(r + ranks - 2 * step, ranks)
            spot = land(phase, j, rank)
            remote(spot, spot, row_send.at[phase, 0], row_recv.at[phase, j, step - 1], (g, partner)).wait_recv()
            pass_copy(phase, j, step).start()

    def row_wait(phase, j):
        where = pl.ds(0, pairs * row_tiles)
        spot = source.at[phase, j, where] if phase < POWERS else everyone.at[j, where]
        remote(spot, spot, row_send.at[phase, 0], row_recv.at[phase, j, pairs - 1], (g, partner)).wait_recv()

    for group in range(groups):
        tile_of = jnp.full((1, table.shape[2]), send_ref[0, group], jnp.int32)
        table[inner, group : group + 1, :] = tile_of.astype(jnp.float32)
    for j in range(chunks):
        keep(0, j, block_ref[:, j * width : (j + 1) * width])

    def clear(slot, carry):
        sums[slot] = jnp.zeros(sums.shape[1:], jnp.float32)
        return carry

    def add_slot(slot, carry):
        sums[slot] = sums[before_ref[slot]] + outgoing[slot].astype(jnp.float32)
        return carry

    lax.fori_loop(0, slots + 1, clear, 0)
    load.wait()
    lax.fori_loop(0, slots, add_slot, 0)
    scales = []
    for row in range(row_tiles):
        degree = degree_ref[row : row + 1, :].astype(jnp.float32)
        scales.append((1.0 / jnp.broadcast_to(degree, (tile, tile))).T)

    def part_of(row, col):
        return (sums[last_ref[row * (local + groups) + col]] * scales[row]).astype(jnp.bfloat16)

    for lane in range(lanes):
        for place in range(LINE):
            rank = place + half * (LINE - 1 - 2 * place)
            for row in range(row_tiles):
                across[lane, rank, row * tile : (row + 1) * tile, :] = part_of(row, local + place * lanes + lane)

    pl.semaphore_wait(barrier, groups + ranks - 2)
    table_copy(far, 3 - inner, 0).start()

    @pl.when(inner == 0)
    def _():
        for j in range(min(AHEAD_END, chunks)):
            up_copy(0, j).start()
        table_copy(hub, 0, 1).start()
        for step in range(lanes):
            give_copy(1, step).start()
        for j in range(min(AHEAD_END, chunks), chunks):
            up_copy(0, j).start()

    @pl.when(inner == 1)
    def _():
        for j in range(min(AHEAD_HUB, chunks)):
            up_copy(0, j).start()
        for step in range(1, lanes):
            give_copy(0, step).start()
        for j in range(early):
            forward_own(j)

    for j in range(chunks):
        row_start(0, j)

    @pl.when(inner == 0)
    def _():
        for j in range(chunks):
            beside(0, j)

    for row in range(row_tiles):
        for col in range(local):
            near[row * tile : (row + 1) * tile, col * tile : (col + 1) * tile] = part_of(row, col)
    def finish(phase, j, in_line):
        row_wait(phase, j)
        if in_line:
            kept = sums[pl.ds(j * row_tiles, row_tiles)].reshape(rows_here, width)
            summed = kept + jnp.dot(
                near[...], source[phase, j, :local].reshape(-1, width),
                preferred_element_type=jnp.float32)
        else:
            spot = source.at[phase, j, pl.ds(local + 1, lanes - 1)]
            remote(spot, spot, side_send.at[phase, 0], side_recv.at[phase, j], at(end, y)).wait_recv()
            matrix = jnp.concatenate(
                [near[...]] + [across[lane_before(step), 0] for step in range(lanes)], axis=1)
            summed = jnp.dot(
                matrix, source[phase, j].reshape(-1, width), preferred_element_type=jnp.float32)
        direct = phase == 0 and j < early and not in_line
        if direct:
            spot = arrived.at[j]
            remote(spot, spot, tile_send.at[0], tile_recv.at[j], at(end, y)).wait_recv()
            matrix = jnp.concatenate(
                [across[lane_before(step), place] for step in range(lanes) for place in range(1, LINE)], axis=1)
            summed += jnp.dot(matrix, arrived[j].reshape(-1, width), preferred_element_type=jnp.float32)
        first = lanes if direct else 1 if in_line else 0
        last = 1 if joined(phase, j) and not in_line else lanes
        if first < last:
            spot = incoming.at[phase, j, pl.ds(first, last - first)]
            remote(spot, spot, part_send.at[j, 0, 0], part_recv.at[phase, j], at(hub, y)).wait_recv()
        for step in range(first, last):
            summed += incoming[phase, j, step].reshape(rows_here, width).astype(jnp.float32)
        current = summed.astype(jnp.bfloat16)
        if phase < POWERS - 1:
            keep(phase + 1, j, current)
            up_copy(phase + 1, j).start()
            if not in_line:
                beside(phase + 1, j)
        else:
            power_sum = current.astype(jnp.float32)
            for past in range(1, POWERS):
                mine = source[past, j, pl.ds(r * row_tiles, row_tiles)].reshape(rows_here, width)
                power_sum = mine.astype(jnp.float32) + power_sum
            keep(phase + 1, j, jnp.log(jnp.maximum(3.0 * power_sum, 1.0)).astype(jnp.bfloat16))
        row_start(phase + 1, j)

    def relay(phase, j):
        line_wait(phase, j, 0, 0)
        relay_copy(phase, j).start()

    def widen(side, step):
        target = (end if side else hub) * lanes + lane_after(step)
        for place in range(side, LINE):
            row = table[place, pl.ds(target, 1), :]
            piece = given[side, step, place]
            for kind in range(row_tiles):
                chosen = jnp.where(row == float(kind), 1.0, 0.0).astype(jnp.bfloat16)
                spot = (place * row_tiles + kind) * tile
                spread[side, step, :, spot : spot + tile] = piece * chosen

    def partial(phase, j, sides):
        if phase > 0 or j >= early:
            line_wait(phase, j, pl.ds(2, 2), 1)
        for side in sides:
            matrix = spread[side, :, :, side * row_tiles * tile :].reshape(lanes * rows_here, -1)
            summed = jnp.dot(
                matrix, line[phase, j, side:].reshape(-1, width), preferred_element_type=jnp.float32)
            for step in reversed(range(lanes)):
                here = summed[step * rows_here : (step + 1) * rows_here]
                if side == 0 and step == 0:
                    sums[pl.ds(j * row_tiles, row_tiles)] = here.reshape(row_tiles, tile, width)
                elif step == 0 and joined(phase, j):
                    sums[pl.ds((chunks + j) * row_tiles, row_tiles)] = here.reshape(row_tiles, tile, width)
                else:
                    if phase > 1 or (phase == 1 and (side == 0 or j >= early)):
                        part_copy(phase - 1, j, side, step).wait_send()
                    where = pl.ds(out_spot(j, side, step), row_tiles)
                    outgoing[where] = here.astype(jnp.bfloat16).reshape(row_tiles, tile, width)
                    part_copy(phase, j, side, step).start()

    def join(phase, j):
        if joined(phase, j):
            spot = incoming.at[phase, j, 0]
            remote(spot, spot, part_send.at[j, 1, 1], joint_recv.at[j], at(hub, y)).wait_recv()
            summed = sums[pl.ds((chunks + j) * row_tiles, row_tiles)] + incoming[phase, j, 0].astype(jnp.float32)
            if j >= early:
                part_copy(phase - 1, j, 1, 0).wait_send()
            outgoing[pl.ds(out_spot(j, 1, 0), row_tiles)] = summed.astype(jnp.bfloat16)
            part_copy(phase, j, 1, 0).start()

    def take(side):
        for step in range(1 - side, lanes):
            spot = given.at[side, step, side:]
            remote(spot, spot, give_send.at[step], give_recv.at[side, step], at(hub, y)).wait_recv()
        for step in range(lanes):
            widen(side, step)

    @pl.when(inner == 1)
    def _():
        given[0, 0] = across[y]
        sent = min(AHEAD_HUB, chunks)
        for j in range(min(AHEAD_END, chunks)):
            relay(0, j)
            if sent < chunks:
                up_copy(0, sent).start()
                sent += 1
        for j in range(sent, chunks):
            up_copy(0, j).start()
        spot = table.at[pl.ds(0, LINE - 1)]
        remote(spot, spot, table_send.at[0], table_recv.at[0], at(far, y)).wait_recv()
        for j in range(early):
            row_pass(0, j)
        for j in range(early):
            forward_rest(j)
            if j == 0:
                take(0)
            partial(0, j, (0,))
            if j > 0:
                finish(0, j - 1, True)
        for j in range(early, chunks):
            row_pass(0, j)
        take(1)
        steps = POWERS * chunks
        for n in range(early, steps + LAG_PASS):
            if n < steps:
                partial(n // chunks, n % chunks, (0, 1))
            m = n - LAG_JOIN
            if early <= m < steps:
                join(m // chunks, m % chunks)
            m = n - LAG_FINISH
            if early - 1 <= m < steps:
                finish(m // chunks, m % chunks, True)
            for m in relays_after(n, n == early, chunks, steps):
                relay(m // chunks, m % chunks)
            m = n - LAG_PASS
            if 0 <= m < steps:
                row_pass(m // chunks + 1, m % chunks)
        for own in (0, 1):
            spot = arrived.at[:, :, pl.ds(0, 1) if own else pl.ds(1, LINE - 2)]
            remote(spot, spot, tile_send.at[1 - own], tile_recv.at[0], at(end, y)).wait_send()
        for phase in range(POWERS):
            spot = line.at[phase, :, 0]
            remote(spot, spot, relay_send.at[phase], line_recv.at[phase, 0, 0], at(far, y)).wait_send()
        for j in range(chunks):
            for side in (0, 1):
                for step in range(1 - side, lanes):
                    part_copy(POWERS - 1, j, side, step).wait_send()
        for step in range(1, lanes):
            give_copy(0, step).wait_send()

    @pl.when(inner == 0)
    def _():
        steps = POWERS * chunks
        for j in range(min(AHEAD_END, chunks)):
            row_pass(0, j)
        for n in range(steps + LAG_END):
            if n < steps:
                finish(n // chunks, n % chunks, False)
            if min(AHEAD_END, chunks) + n < chunks:
                row_pass(0, min(AHEAD_END, chunks) + n)
            m = n - LAG_END
            if m >= 0:
                row_pass(m // chunks + 1, m % chunks)
        for step in range(lanes):
            give_copy(1, step).wait_send()
        for phase in range(POWERS):
            for step in range(1, lanes):
                spot = outgoing.at[pl.ds(0, chunks)]
                remote(spot, spot, side_send.at[phase, step], side_recv.at[phase, 0], at(end, y)).wait_send()
        table_copy(hub, 0, 1).wait_send()

    def row_sent(phase):
        for step in range(pairs):
            spot = span(phase, r)
            remote(spot, spot, row_send.at[phase, step], row_recv.at[phase, 0, 0], (g, partner)).wait_send()
        for step in range(1, pairs):
            spot = span(phase, lax.rem(r + ranks - 2 * step, ranks))
            remote(spot, spot, pass_send.at[phase, step - 1], row_recv.at[phase, 0, 0], (g, partner)).wait_send()

    table_copy(far, 3 - inner, 0).wait_send()
    for phase in range(POWERS):
        spot = span(phase, r)
        remote(spot, spot, up_send.at[phase], line_recv.at[phase, 0, 0], at(onward, y)).wait_send()
        row_sent(phase)
    for j in range(chunks):
        row_wait(POWERS, j)
        pltpu.make_async_copy(everyone.at[j], gathered_hbm.at[j], out_sem.at[0]).start()
    row_sent(POWERS)
    pltpu.make_async_copy(everyone, gathered_hbm, out_sem.at[0]).wait()


def gram_kernel(ranks, gathered_hbm, logs_hbm, gram_hbm, gathered, mine, logs, gram, in_sem, logs_sem, out_sem):
    chunks, local, tile, width = gathered.shape
    rows_here = local // ranks * tile
    r = lax.axis_index("row")
    each = chunks // ranks

    def in_copy(j):
        return pltpu.make_async_copy(gathered_hbm.at[j], gathered.at[j], in_sem.at[j])

    def out_copy(k):
        where = pl.ds(pl.multiple_of(k * each * width, width), each * width)
        return pltpu.make_async_copy(gram.at[:, where], gram_hbm.at[:, where], out_sem.at[k])

    def logs_copy(k):
        where = pl.ds(pl.multiple_of(k * each * width, width), each * width)
        return pltpu.make_async_copy(logs.at[:, where], logs_hbm.at[:, where], logs_sem.at[k])

    for j in range(chunks):
        in_copy(lax.rem(r * each + j, chunks)).start()
    for j in range(each):
        in_copy(r * each + j).wait()
        mine[j * width : (j + 1) * width, :] = gathered[r * each + j].reshape(-1, width).T
    own = pl.ds(r * (local // ranks), local // ranks)
    for step in range(ranks):
        k = lax.rem(r + step, ranks)
        if step:
            for j in range(each):
                in_copy(k * each + j).wait()
        block = jnp.concatenate([gathered[k * each + j].reshape(-1, width) for j in range(each)], axis=1)
        part = jnp.dot(mine[...], block, preferred_element_type=jnp.float32) / (rows_here * ranks)
        where = pl.ds(pl.multiple_of(k * each * width, width), each * width)
        gram[:, where] = part
        out_copy(k).start()
        logs[:, where] = jnp.concatenate(
            [gathered[k * each + j, own].reshape(rows_here, width) for j in range(each)], axis=1)
        logs_copy(k).start()
    for k in range(ranks):
        out_copy(k).wait()
        logs_copy(k).wait()


def body(block, degree, tile_values, tile_rows, tile_cols, tile_count, send_tiles):
    rows_here, width = block.shape
    tile = tile_values.shape[1]
    row_tiles = rows_here // tile
    ranks = lax.axis_size("row")
    groups = lax.axis_size("grp")
    local = ranks * row_tiles
    lanes = groups // LINE
    sources = local + groups
    smem = pl.BlockSpec(memory_space=pltpu.SMEM)
    vmem = pl.BlockSpec(memory_space=pltpu.VMEM)
    slots = tile_values.shape[0]
    before, last = pl.pallas_call(
        functools.partial(order_kernel, sources),
        out_shape=(
            jax.ShapeDtypeStruct((slots,), jnp.int32),
            jax.ShapeDtypeStruct((row_tiles * sources,), jnp.int32),
        ),
        in_specs=[smem, smem, smem],
        out_specs=(smem, smem),
        name="order",
    )(tile_rows, tile_cols, tile_count)
    share = width // ranks
    early = max(1, min(FORWARD, 8 // lanes))
    pairs = ranks // 2
    chunks = max(ranks, CHUNKS)
    part = width // chunks
    dma = pltpu.SemaphoreType.DMA
    half = jnp.bfloat16
    anywhere = pl.BlockSpec(memory_space=pl.ANY)
    gathered = pl.pallas_call(
        functools.partial(step_kernel, groups, ranks),
        out_shape=jax.ShapeDtypeStruct((chunks, local, tile, part), half),
        in_specs=[smem, smem, smem, vmem, anywhere, vmem],
        out_specs=anywhere,
        scratch_shapes=[
            dma,
            pltpu.VMEM((slots + 1, tile, tile), jnp.float32),
            pltpu.VMEM((rows_here, local * tile), half),
            pltpu.VMEM((lanes, LINE, rows_here, tile), half),
            pltpu.VMEM((LINE, groups, tile), jnp.float32),
            pltpu.VMEM((2, lanes, LINE, rows_here, tile), half),
            pltpu.VMEM((2, lanes, rows_here, LINE * row_tiles * tile), half),
            pltpu.VMEM((POWERS, chunks, local + lanes, tile, part), half),
            pltpu.VMEM((early, lanes, LINE - 1, tile, part), half),
            pltpu.VMEM((POWERS, chunks, LINE, row_tiles, tile, part), half),
            pltpu.VMEM((chunks * 2 * lanes * row_tiles, tile, part), half),
            pltpu.VMEM((POWERS, chunks, lanes, row_tiles, tile, part), half),
            pltpu.VMEM((chunks, local, tile, part), half),
            dma((POWERS + 1, pairs)),
            dma((POWERS + 1, chunks, pairs)),
            dma((POWERS + 1, pairs)),
            dma((POWERS,)),
            dma((POWERS,)),
            dma((POWERS, chunks, 2)),
            dma((chunks, 2, lanes)),
            dma((POWERS, chunks)),
            dma((lanes,)),
            dma((2, lanes)),
            dma((2,)),
            dma((1,)),
            dma((POWERS, lanes)),
            dma((POWERS, chunks)),
            dma((2,)),
            dma((early,)),
            dma((chunks,)),
            dma((1,)),
        ],
        compiler_params=pltpu.CompilerParams(
            collective_id=0, has_side_effects=True, vmem_limit_bytes=67043328),
        name="step",
    )(send_tiles, before, last, degree.reshape(row_tiles, tile), tile_values, block)
    return tuple(pl.pallas_call(
        functools.partial(gram_kernel, ranks),
        out_shape=(
            jax.ShapeDtypeStruct((rows_here, width), half),
            jax.ShapeDtypeStruct((share, width), jnp.float32),
        ),
        in_specs=[anywhere],
        out_specs=(anywhere, anywhere),
        scratch_shapes=[
            pltpu.VMEM(gathered.shape, half),
            pltpu.VMEM((share, rows_here * ranks), half),
            pltpu.VMEM((rows_here, width), half),
            pltpu.VMEM((share, width), jnp.float32),
            dma((chunks,)),
            dma((ranks,)),
            dma((ranks,)),
        ],
        name="gram",
    )(gathered))


def solution(mesh):
    placed = (
        P(("grp", "row"), None),
        P(("grp", "row")),
        P(("grp", "row"), None, None),
        P(("grp", "row")),
        P(("grp", "row")),
        P(("grp", "row")),
        P(("grp", "row"), None),
    )
    return jax.shard_map(
        body,
        mesh=mesh,
        in_specs=placed,
        out_specs=(P(("grp", "row"), None), P(("grp", "row"), None)),
        check_vma=False,
    )
```

```python
import functools

import jax
import jax.numpy as jnp
from jax import lax
from jax.experimental import pallas as pl
from jax.experimental.pallas import tpu as pltpu
from jax.sharding import PartitionSpec as P

POWERS = 2
LINE = 4
CHUNKS = 8
AHEAD_HUB = 3
AHEAD_END = 4
FORWARD = 3
LAG_JOIN = 2
LAG_FINISH = 6
LAG_RELAY = 4
AHEAD_RELAY = 3
LAG_PASS = 8
LAG_END = 3
MESH = pl.DeviceIdType.MESH


def relays_after(n, first, chunks, steps):
    near = range(min(AHEAD_END, chunks) if first else n + AHEAD_RELAY, n + AHEAD_RELAY + 1)
    later = range(chunks if first else n + LAG_RELAY, n + LAG_RELAY + 1)
    return [m for m in near if m < chunks] + [m for m in later if chunks <= m < steps]


def order_kernel(sources, rows_ref, cols_ref, count_ref, before_ref, last_ref):
    slots = rows_ref.shape[0]

    def clear(place, carry):
        last_ref[place] = slots
        return carry

    def skip(slot, carry):
        before_ref[slot] = slots
        return carry

    def link(slot, carry):
        place = rows_ref[slot] * sources + cols_ref[slot]
        before_ref[slot] = last_ref[place]
        last_ref[place] = slot
        return carry

    lax.fori_loop(0, last_ref.shape[0], clear, 0)
    lax.fori_loop(0, slots, skip, 0)
    lax.fori_loop(0, count_ref[0], link, 0)


def step_kernel(
    groups, ranks, send_ref, before_ref, last_ref, degree_ref, values_hbm, block_ref, gathered_hbm,
    values_sem, sums, near, across, table, given, spread,
    source, arrived, line, outgoing, incoming, everyone,
    row_send, row_recv, pass_send, up_send, relay_send, line_recv, part_send, part_recv,
    give_send, give_recv, table_send, table_recv, side_send, side_recv, tile_send, tile_recv, joint_recv, out_sem,
):
    chunks, local, tile, width = everyone.shape
    early = arrived.shape[0]
    row_tiles = line.shape[3]
    rows_here = row_tiles * tile
    lanes = groups // LINE
    g = lax.axis_index("grp")
    r = lax.axis_index("row")
    z = g // lanes
    y = lax.rem(g, lanes)
    half = z // 2
    inner = lax.rem(z + half, 2)
    hub = 1 + half
    far = 2 - half
    end = 3 * half
    onward = hub + inner * (far - hub)
    core = lax.rem(r, 2)
    partner = r + 1 - 2 * core
    pairs = ranks // 2

    slots = values_hbm.shape[0]
    load = pltpu.make_async_copy(values_hbm, outgoing.at[pl.ds(0, slots)], values_sem)
    load.start()

    def at(place, lane):
        return (place * lanes + lane, r)

    def lane_after(step):
        return lax.rem(y + step, lanes)

    def lane_before(step):
        return lax.rem(y + lanes - step, lanes)

    def same_core(step):
        return lax.rem(r + 2 * step, ranks)

    barrier = pltpu.get_barrier_semaphore()
    for step in range(1, groups):
        pl.semaphore_signal(barrier, inc=1, device_id=(lax.rem(g + step, groups), r), device_id_type=MESH)
    for step in range(1, ranks):
        pl.semaphore_signal(barrier, inc=1, device_id=(g, lax.rem(r + step, ranks)), device_id_type=MESH)

    def remote(src, dst, send_sem, recv_sem, to):
        return pltpu.make_async_remote_copy(
            src_ref=src, dst_ref=dst, send_sem=send_sem, recv_sem=recv_sem, device_id=to, device_id_type=MESH)

    def land(phase, j, rank):
        where = pl.ds(rank * row_tiles, row_tiles)
        return source.at[phase, j, where] if phase < POWERS else everyone.at[j, where]

    def span(phase, rank):
        where = pl.ds(rank * row_tiles, row_tiles)
        return source.at[phase, :, where] if phase < POWERS else everyone.at[:, where]

    def row_copy(phase, j, step):
        spot = land(phase, j, r)
        to = same_core(step) if step else partner
        arrival = step - 1 if step else pairs - 1
        return remote(spot, spot, row_send.at[phase, step], row_recv.at[phase, j, arrival], (g, to))

    def pass_copy(phase, j, step):
        spot = land(phase, j, lax.rem(r + ranks - 2 * step, ranks))
        return remote(
            spot, spot, pass_send.at[phase, step - 1], row_recv.at[phase, j, pairs - 1], (g, partner))

    def up_copy(phase, j):
        return remote(
            land(phase, j, r), line.at[phase, j, 2 * inner], up_send.at[phase], line_recv.at[phase, j, inner],
            at(onward, y))

    def relay_copy(phase, j):
        return remote(
            line.at[phase, j, 0], line.at[phase, j, 3], relay_send.at[phase], line_recv.at[phase, j, 1],
            at(far, y))

    def line_wait(phase, j, where, kind):
        spot = line.at[phase, j, where]
        remote(spot, spot, relay_send.at[phase], line_recv.at[phase, j, kind], at(far, y)).wait_recv()

    def out_spot(j, side, step):
        return ((j * 2 + side) * lanes + step) * row_tiles

    def side_copy(phase, j, step):
        return remote(
            outgoing.at[out_spot(j, phase, step)], source.at[phase, j, local + step], side_send.at[phase, step],
            side_recv.at[phase, j], at(end, lane_after(step)))

    def tile_copy(j, step, own):
        where = pl.ds(0, 1) if own else pl.ds(1, LINE - 2)
        return remote(
            arrived.at[j, step, where], arrived.at[j, step, where], tile_send.at[1 - own], tile_recv.at[j],
            at(end, lane_after(step)))

    def joined(phase, j):
        return lanes == 2 and phase == POWERS - 1 and j % 2 == 0 and j < chunks - 2

    def part_copy(phase, j, side, step):
        if side and step and joined(phase, j):
            return remote(
                outgoing.at[pl.ds(out_spot(j, side, step), row_tiles)], incoming.at[phase, j, 0],
                part_send.at[j, side, step], joint_recv.at[j], at(hub, lane_after(step)))
        return remote(
            outgoing.at[pl.ds(out_spot(j, side, step), row_tiles)], incoming.at[phase, j, step],
            part_send.at[j, side, step], part_recv.at[phase, j],
            at(end if side else hub, lane_after(step)))

    def give_copy(side, step):
        return remote(
            across.at[lane_before(step), side:], given.at[side, step, side:],
            give_send.at[step], give_recv.at[side, step], at(hub, lane_before(step)))

    def table_copy(to, place, sem):
        return remote(table.at[inner], table.at[place], table_send.at[sem], table_recv.at[0], at(to, y))

    def keep(phase, j, value):
        tiles = value.reshape(row_tiles, tile, width)
        if phase < POWERS:
            source[phase, j, pl.ds(r * row_tiles, row_tiles)] = tiles
            line[phase, j, 1] = tiles
        else:
            everyone[j, pl.ds(r * row_tiles, row_tiles)] = tiles

    def wanted(phase, j, group):
        picked = source[phase, j, r * row_tiles]
        for kind in range(1, row_tiles):
            picked = jnp.where(send_ref[0, group] == kind, source[phase, j, r * row_tiles + kind], picked)
        return picked

    def beside(phase, j):
        for step in range(1, lanes):
            outgoing[out_spot(j, phase, step)] = wanted(phase, j, end * lanes + lane_after(step))
            side_copy(phase, j, step).start()
        source[phase, j, local] = wanted(phase, j, g)

    def forward_own(j):
        for step in range(lanes):
            arrived[j, step, 0] = wanted(0, j, end * lanes + lane_after(step))
            tile_copy(j, step, 1).start()

    def forward_rest(j):
        line_wait(0, j, pl.ds(2, 2), 1)
        for step in range(lanes):
            for place in range(2, LINE):
                row = table[place, pl.ds(end * lanes + lane_after(step), 1), :]
                picked = line[0, j, place, 0]
                for kind in range(1, row_tiles):
                    chosen = jnp.where(row == float(kind), 1.0, 0.0).astype(jnp.bfloat16)
                    picked = picked * (1 - chosen) + line[0, j, place, kind] * chosen
                arrived[j, step, place - 1] = picked
            tile_copy(j, step, 0).start()

    def row_start(phase, j):
        for step in (*range(1, pairs), 0):
            row_copy(phase, j, step).start()

    def row_pass(phase, j):
        for step in range(1, pairs):
            rank = lax.rem(r + ranks - 2 * step, ranks)
            spot = land(phase, j, rank)
            remote(spot, spot, row_send.at[phase, 0], row_recv.at[phase, j, step - 1], (g, partner)).wait_recv()
            pass_copy(phase, j, step).start()

    def row_wait(phase, j):
        where = pl.ds(0, pairs * row_tiles)
        spot = source.at[phase, j, where] if phase < POWERS else everyone.at[j, where]
        remote(spot, spot, row_send.at[phase, 0], row_recv.at[phase, j, pairs - 1], (g, partner)).wait_recv()

    for group in range(groups):
        tile_of = jnp.full((1, table.shape[2]), send_ref[0, group], jnp.int32)
        table[inner, group : group + 1, :] = tile_of.astype(jnp.float32)
    for j in range(chunks):
        keep(0, j, block_ref[:, j * width : (j + 1) * width])

    def clear(slot, carry):
        sums[slot] = jnp.zeros(sums.shape[1:], jnp.float32)
        return carry

    def add_slot(slot, carry):
        sums[slot] = sums[before_ref[slot]] + outgoing[slot].astype(jnp.float32)
        return carry

    lax.fori_loop(0, slots + 1, clear, 0)
    load.wait()
    lax.fori_loop(0, slots, add_slot, 0)
    scales = []
    for row in range(row_tiles):
        degree = degree_ref[row : row + 1, :].astype(jnp.float32)
        scales.append((1.0 / jnp.broadcast_to(degree, (tile, tile))).T)

    def part_of(row, col):
        return (sums[last_ref[row * (local + groups) + col]] * scales[row]).astype(jnp.bfloat16)

    for lane in range(lanes):
        for place in range(LINE):
            rank = place + half * (LINE - 1 - 2 * place)
            for row in range(row_tiles):
                across[lane, rank, row * tile : (row + 1) * tile, :] = part_of(row, local + place * lanes + lane)

    pl.semaphore_wait(barrier, groups + ranks - 2)
    table_copy(far, 3 - inner, 0).start()

    @pl.when(inner == 0)
    def _():
        for j in range(min(AHEAD_END, chunks)):
            up_copy(0, j).start()
        table_copy(hub, 0, 1).start()
        for step in range(lanes):
            give_copy(1, step).start()
        for j in range(min(AHEAD_END, chunks), chunks):
            up_copy(0, j).start()

    @pl.when(inner == 1)
    def _():
        for j in range(min(AHEAD_HUB, chunks)):
            up_copy(0, j).start()
        for step in range(1, lanes):
            give_copy(0, step).start()
        for j in range(early):
            forward_own(j)

    for j in range(chunks):
        row_start(0, j)

    @pl.when(inner == 0)
    def _():
        for j in range(chunks):
            beside(0, j)

    for row in range(row_tiles):
        for col in range(local):
            near[row * tile : (row + 1) * tile, col * tile : (col + 1) * tile] = part_of(row, col)
    def finish(phase, j, in_line):
        row_wait(phase, j)
        if in_line:
            kept = sums[pl.ds(j * row_tiles, row_tiles)].reshape(rows_here, width)
            summed = kept + jnp.dot(
                near[...], source[phase, j, :local].reshape(-1, width),
                preferred_element_type=jnp.float32)
        else:
            spot = source.at[phase, j, pl.ds(local + 1, lanes - 1)]
            remote(spot, spot, side_send.at[phase, 0], side_recv.at[phase, j], at(end, y)).wait_recv()
            matrix = jnp.concatenate(
                [near[...]] + [across[lane_before(step), 0] for step in range(lanes)], axis=1)
            summed = jnp.dot(
                matrix, source[phase, j].reshape(-1, width), preferred_element_type=jnp.float32)
        direct = phase == 0 and j < early and not in_line
        if direct:
            spot = arrived.at[j]
            remote(spot, spot, tile_send.at[0], tile_recv.at[j], at(end, y)).wait_recv()
            matrix = jnp.concatenate(
                [across[lane_before(step), place] for step in range(lanes) for place in range(1, LINE)], axis=1)
            summed += jnp.dot(matrix, arrived[j].reshape(-1, width), preferred_element_type=jnp.float32)
        first = lanes if direct else 1 if in_line else 0
        last = 1 if joined(phase, j) and not in_line else lanes
        if first < last:
            spot = incoming.at[phase, j, pl.ds(first, last - first)]
            remote(spot, spot, part_send.at[j, 0, 0], part_recv.at[phase, j], at(hub, y)).wait_recv()
        for step in range(first, last):
            summed += incoming[phase, j, step].reshape(rows_here, width).astype(jnp.float32)
        current = summed.astype(jnp.bfloat16)
        if phase < POWERS - 1:
            keep(phase + 1, j, current)
            up_copy(phase + 1, j).start()
            if not in_line:
                beside(phase + 1, j)
        else:
            power_sum = current.astype(jnp.float32)
            for past in range(1, POWERS):
                mine = source[past, j, pl.ds(r * row_tiles, row_tiles)].reshape(rows_here, width)
                power_sum = mine.astype(jnp.float32) + power_sum
            keep(phase + 1, j, jnp.log(jnp.maximum(3.0 * power_sum, 1.0)).astype(jnp.bfloat16))
        row_start(phase + 1, j)

    def relay(phase, j):
        line_wait(phase, j, 0, 0)
        relay_copy(phase, j).start()

    def widen(side, step):
        target = (end if side else hub) * lanes + lane_after(step)
        for place in range(side, LINE):
            row = table[place, pl.ds(target, 1), :]
            piece = given[side, step, place]
            for kind in range(row_tiles):
                chosen = jnp.where(row == float(kind), 1.0, 0.0).astype(jnp.bfloat16)
                spot = (place * row_tiles + kind) * tile
                spread[side, step, :, spot : spot + tile] = piece * chosen

    def partial(phase, j, sides):
        if phase > 0 or j >= early:
            line_wait(phase, j, pl.ds(2, 2), 1)
        for side in sides:
            matrix = spread[side, :, :, side * row_tiles * tile :].reshape(lanes * rows_here, -1)
            summed = jnp.dot(
                matrix, line[phase, j, side:].reshape(-1, width), preferred_element_type=jnp.float32)
            for step in reversed(range(lanes)):
                here = summed[step * rows_here : (step + 1) * rows_here]
                if side == 0 and step == 0:
                    sums[pl.ds(j * row_tiles, row_tiles)] = here.reshape(row_tiles, tile, width)
                elif step == 0 and joined(phase, j):
                    sums[pl.ds((chunks + j) * row_tiles, row_tiles)] = here.reshape(row_tiles, tile, width)
                else:
                    if phase > 1 or (phase == 1 and (side == 0 or j >= early)):
                        part_copy(phase - 1, j, side, step).wait_send()
                    where = pl.ds(out_spot(j, side, step), row_tiles)
                    outgoing[where] = here.astype(jnp.bfloat16).reshape(row_tiles, tile, width)
                    part_copy(phase, j, side, step).start()

    def join(phase, j):
        if joined(phase, j):
            spot = incoming.at[phase, j, 0]
            remote(spot, spot, part_send.at[j, 1, 1], joint_recv.at[j], at(hub, y)).wait_recv()
            summed = sums[pl.ds((chunks + j) * row_tiles, row_tiles)] + incoming[phase, j, 0].astype(jnp.float32)
            if j >= early:
                part_copy(phase - 1, j, 1, 0).wait_send()
            outgoing[pl.ds(out_spot(j, 1, 0), row_tiles)] = summed.astype(jnp.bfloat16)
            part_copy(phase, j, 1, 0).start()

    def take(side):
        for step in range(1 - side, lanes):
            spot = given.at[side, step, side:]
            remote(spot, spot, give_send.at[step], give_recv.at[side, step], at(hub, y)).wait_recv()
        for step in range(lanes):
            widen(side, step)

    @pl.when(inner == 1)
    def _():
        given[0, 0] = across[y]
        sent = min(AHEAD_HUB, chunks)
        for j in range(min(AHEAD_END, chunks)):
            relay(0, j)
            if sent < chunks:
                up_copy(0, sent).start()
                sent += 1
        for j in range(sent, chunks):
            up_copy(0, j).start()
        spot = table.at[pl.ds(0, LINE - 1)]
        remote(spot, spot, table_send.at[0], table_recv.at[0], at(far, y)).wait_recv()
        for j in range(early):
            row_pass(0, j)
        for j in range(early):
            forward_rest(j)
            if j == 0:
                take(0)
            partial(0, j, (0,))
            if j > 0:
                finish(0, j - 1, True)
        for j in range(early, chunks):
            row_pass(0, j)
        take(1)
        steps = POWERS * chunks
        for n in range(early, steps + LAG_PASS):
            if n < steps:
                partial(n // chunks, n % chunks, (0, 1))
            m = n - LAG_JOIN
            if early <= m < steps:
                join(m // chunks, m % chunks)
            m = n - LAG_FINISH
            if early - 1 <= m < steps:
                finish(m // chunks, m % chunks, True)
            for m in relays_after(n, n == early, chunks, steps):
                relay(m // chunks, m % chunks)
            m = n - LAG_PASS
            if 0 <= m < steps:
                row_pass(m // chunks + 1, m % chunks)
        for own in (0, 1):
            spot = arrived.at[:, :, pl.ds(0, 1) if own else pl.ds(1, LINE - 2)]
            remote(spot, spot, tile_send.at[1 - own], tile_recv.at[0], at(end, y)).wait_send()
        for phase in range(POWERS):
            spot = line.at[phase, :, 0]
            remote(spot, spot, relay_send.at[phase], line_recv.at[phase, 0, 0], at(far, y)).wait_send()
        for j in range(chunks):
            for side in (0, 1):
                for step in range(1 - side, lanes):
                    part_copy(POWERS - 1, j, side, step).wait_send()
        for step in range(1, lanes):
            give_copy(0, step).wait_send()

    @pl.when(inner == 0)
    def _():
        steps = POWERS * chunks
        for j in range(min(AHEAD_END, chunks)):
            row_pass(0, j)
        for n in range(steps + LAG_END):
            if n < steps:
                finish(n // chunks, n % chunks, False)
            if min(AHEAD_END, chunks) + n < chunks:
                row_pass(0, min(AHEAD_END, chunks) + n)
            m = n - LAG_END
            if m >= 0:
                row_pass(m // chunks + 1, m % chunks)
        for step in range(lanes):
            give_copy(1, step).wait_send()
        for phase in range(POWERS):
            for step in range(1, lanes):
                spot = outgoing.at[pl.ds(0, chunks)]
                remote(spot, spot, side_send.at[phase, step], side_recv.at[phase, 0], at(end, y)).wait_send()
        table_copy(hub, 0, 1).wait_send()

    def row_sent(phase):
        for step in range(pairs):
            spot = span(phase, r)
            remote(spot, spot, row_send.at[phase, step], row_recv.at[phase, 0, 0], (g, partner)).wait_send()
        for step in range(1, pairs):
            spot = span(phase, lax.rem(r + ranks - 2 * step, ranks))
            remote(spot, spot, pass_send.at[phase, step - 1], row_recv.at[phase, 0, 0], (g, partner)).wait_send()

    table_copy(far, 3 - inner, 0).wait_send()
    for phase in range(POWERS):
        spot = span(phase, r)
        remote(spot, spot, up_send.at[phase], line_recv.at[phase, 0, 0], at(onward, y)).wait_send()
        row_sent(phase)
    for j in range(chunks):
        row_wait(POWERS, j)
        pltpu.make_async_copy(everyone.at[j], gathered_hbm.at[j], out_sem.at[0]).start()
    row_sent(POWERS)
    pltpu.make_async_copy(everyone, gathered_hbm, out_sem.at[0]).wait()


def gram_kernel(ranks, gathered_hbm, logs_hbm, gram_hbm, gathered, mine, logs, gram, in_sem, logs_sem, out_sem):
    chunks, local, tile, width = gathered.shape
    rows_here = local // ranks * tile
    r = lax.axis_index("row")
    each = chunks // ranks

    def in_copy(j):
        return pltpu.make_async_copy(gathered_hbm.at[j], gathered.at[j], in_sem.at[j])

    def out_copy(k):
        where = pl.ds(pl.multiple_of(k * each * width, width), each * width)
        return pltpu.make_async_copy(gram.at[:, where], gram_hbm.at[:, where], out_sem.at[k])

    def logs_copy(k):
        where = pl.ds(pl.multiple_of(k * each * width, width), each * width)
        return pltpu.make_async_copy(logs.at[:, where], logs_hbm.at[:, where], logs_sem.at[k])

    for j in range(chunks):
        in_copy(lax.rem(r * each + j, chunks)).start()
    for j in range(each):
        in_copy(r * each + j).wait()
        mine[j * width : (j + 1) * width, :] = gathered[r * each + j].reshape(-1, width).T
    own = pl.ds(r * (local // ranks), local // ranks)
    for step in range(ranks):
        k = lax.rem(r + step, ranks)
        if step:
            for j in range(each):
                in_copy(k * each + j).wait()
        block = jnp.concatenate([gathered[k * each + j].reshape(-1, width) for j in range(each)], axis=1)
        part = jnp.dot(mine[...], block, preferred_element_type=jnp.float32) / (rows_here * ranks)
        where = pl.ds(pl.multiple_of(k * each * width, width), each * width)
        gram[:, where] = part
        out_copy(k).start()
        logs[:, where] = jnp.concatenate(
            [gathered[k * each + j, own].reshape(rows_here, width) for j in range(each)], axis=1)
        logs_copy(k).start()
    for k in range(ranks):
        out_copy(k).wait()
        logs_copy(k).wait()


def body(block, degree, tile_values, tile_rows, tile_cols, tile_count, send_tiles):
    rows_here, width = block.shape
    tile = tile_values.shape[1]
    row_tiles = rows_here // tile
    ranks = lax.axis_size("row")
    groups = lax.axis_size("grp")
    local = ranks * row_tiles
    lanes = groups // LINE
    sources = local + groups
    smem = pl.BlockSpec(memory_space=pltpu.SMEM)
    vmem = pl.BlockSpec(memory_space=pltpu.VMEM)
    slots = tile_values.shape[0]
    before, last = pl.pallas_call(
        functools.partial(order_kernel, sources),
        out_shape=(
            jax.ShapeDtypeStruct((slots,), jnp.int32),
            jax.ShapeDtypeStruct((row_tiles * sources,), jnp.int32),
        ),
        in_specs=[smem, smem, smem],
        out_specs=(smem, smem),
        name="order",
    )(tile_rows, tile_cols, tile_count)
    share = width // ranks
    early = max(1, min(FORWARD, 8 // lanes))
    pairs = ranks // 2
    chunks = max(ranks, CHUNKS)
    part = width // chunks
    dma = pltpu.SemaphoreType.DMA
    half = jnp.bfloat16
    anywhere = pl.BlockSpec(memory_space=pl.ANY)
    gathered = pl.pallas_call(
        functools.partial(step_kernel, groups, ranks),
        out_shape=jax.ShapeDtypeStruct((chunks, local, tile, part), half),
        in_specs=[smem, smem, smem, vmem, anywhere, vmem],
        out_specs=anywhere,
        scratch_shapes=[
            dma,
            pltpu.VMEM((slots + 1, tile, tile), jnp.float32),
            pltpu.VMEM((rows_here, local * tile), half),
            pltpu.VMEM((lanes, LINE, rows_here, tile), half),
            pltpu.VMEM((LINE, groups, tile), jnp.float32),
            pltpu.VMEM((2, lanes, LINE, rows_here, tile), half),
            pltpu.VMEM((2, lanes, rows_here, LINE * row_tiles * tile), half),
            pltpu.VMEM((POWERS, chunks, local + lanes, tile, part), half),
            pltpu.VMEM((early, lanes, LINE - 1, tile, part), half),
            pltpu.VMEM((POWERS, chunks, LINE, row_tiles, tile, part), half),
            pltpu.VMEM((chunks * 2 * lanes * row_tiles, tile, part), half),
            pltpu.VMEM((POWERS, chunks, lanes, row_tiles, tile, part), half),
            pltpu.VMEM((chunks, local, tile, part), half),
            dma((POWERS + 1, pairs)),
            dma((POWERS + 1, chunks, pairs)),
            dma((POWERS + 1, pairs)),
            dma((POWERS,)),
            dma((POWERS,)),
            dma((POWERS, chunks, 2)),
            dma((chunks, 2, lanes)),
            dma((POWERS, chunks)),
            dma((lanes,)),
            dma((2, lanes)),
            dma((2,)),
            dma((1,)),
            dma((POWERS, lanes)),
            dma((POWERS, chunks)),
            dma((2,)),
            dma((early,)),
            dma((chunks,)),
            dma((1,)),
        ],
        compiler_params=pltpu.CompilerParams(
            collective_id=0, has_side_effects=True, vmem_limit_bytes=67043328),
        name="step",
    )(send_tiles, before, last, degree.reshape(row_tiles, tile), tile_values, block)
    return tuple(pl.pallas_call(
        functools.partial(gram_kernel, ranks),
        out_shape=(
            jax.ShapeDtypeStruct((rows_here, width), half),
            jax.ShapeDtypeStruct((share, width), jnp.float32),
        ),
        in_specs=[anywhere],
        out_specs=(anywhere, anywhere),
        scratch_shapes=[
            pltpu.VMEM(gathered.shape, half),
            pltpu.VMEM((share, rows_here * ranks), half),
            pltpu.VMEM((rows_here, width), half),
            pltpu.VMEM((share, width), jnp.float32),
            dma((chunks,)),
            dma((ranks,)),
            dma((ranks,)),
        ],
        name="gram",
    )(gathered))


def solution(mesh):
    placed = (
        P(("grp", "row"), None),
        P(("grp", "row")),
        P(("grp", "row"), None, None),
        P(("grp", "row")),
        P(("grp", "row")),
        P(("grp", "row")),
        P(("grp", "row"), None),
    )
    return jax.shard_map(
        body,
        mesh=mesh,
        in_specs=placed,
        out_specs=(P(("grp", "row"), None), P(("grp", "row"), None)),
        check_vma=False,
    )
```
